128 devices in a mesh: row: 8 (over x, y_hi), col: 16 (over y_lo, z, core).
Axes of the slice: x: 4, y: 4 (y_hi: 2, y_lo: 2; y = y_hi * 2 + y_lo), z: 4, core: 2. Of those that a mesh axis runs over, the one named last changes fastest.
Arguments:
- b_values: bfloat16 [4096, 12288], P('row', 'col'), may hold values from -0.09375 to 0.09375
- tile_mask: int32 [16, 48], replicated, may hold values 0 or 1
Outputs:
- factored: float32 [12288, 12288], P('row', 'col')
The draws below stay inside these ranges and needn't reach their ends.
Inputs may be any that keep to these rules, and one draw needn't show every extreme that they name: tile_mask[i, j] is 1 where tile (i, j) of B is kept and 0 where it is empty.
All inputs are finite; a program needn't handle non-finite values.
Results may differ from the reference program's by a relative error of at most 0.0017.
Values may be sent and summed in bfloat16 or wider, within the bound.
A program may use at most 128 MiB of HBM per device.

```python
import jax
import jax.numpy as jnp
from jax import lax

AUX = 12288
TILE = 256
PANEL = 512
ROWS = 4096


def place_ends(result, stream_key, least, high):
    longest = result.shape.index(max(result.shape))
    spots = []
    for shift in (0, 1):
        where = [jax.random.randint(jax.random.fold_in(stream_key, axis), (), 0, length) for axis, length in enumerate(result.shape)]
        where[longest] = (where[longest] + shift) % result.shape[longest]
        spots.append(tuple(where))
    return result.at[spots[0]].set(least).at[spots[1]].set(high)


def levels(rng, extent, shards, smallest, largest):
    def one(axis_at, parts):
        draws = jax.random.uniform(jax.random.fold_in(jax.random.fold_in(rng, 6), axis_at), (parts,), jnp.float32, smallest / len(shards), largest / len(shards))
        return jnp.repeat(jnp.exp(draws), extent[axis_at] // parts).reshape((-1,) + (1,) * (len(extent) - axis_at - 1))

    gain = one(*shards[0])
    for cut in shards[1:]:
        gain = gain * one(*cut)
    return gain


def gaussian(own_key, shape, scale, reach, pieces=(), held_as=jnp.bfloat16):
    drawn = jax.random.normal(own_key, shape, jnp.float32) * scale
    if len(pieces) > 0:
        drawn = levels(own_key, shape, pieces, -0.22, 0.18) * drawn
    return jnp.clip(drawn, min=-reach, max=reach).astype(held_as)


def setup_inputs(seed: int = 0) -> dict:
    arg_keys = jax.random.split(jax.random.key(seed), 3)
    return {
        "b_values": gaussian(arg_keys[0], (ROWS, AUX), ROWS ** -0.5, 0.09375, ((0, 8), (1, 16))),
        "tile_mask": place_ends((jax.random.randint(arg_keys[1], (ROWS // TILE, AUX // TILE), 0, 4) < 3).astype(jnp.int32), jax.random.fold_in(arg_keys[1], 1), 0, 1),
    }


def expand_tiles(blocks):
    return jnp.repeat(jnp.repeat(blocks, TILE, axis=0), TILE, axis=1)

def factor_top(corner, panel):
    width = corner.shape[0]
    updated = corner
    factor = jnp.zeros_like(corner)
    for number in range(width // panel):
        lower_edge = number * panel
        upper_edge = lower_edge + panel
        diagonal_block = jnp.linalg.cholesky(updated[lower_edge:upper_edge, lower_edge:upper_edge])
        below = jax.scipy.linalg.solve_triangular(diagonal_block, updated[upper_edge:, lower_edge:upper_edge].T, lower=True).T
        factor = factor.at[lower_edge:upper_edge, lower_edge:upper_edge].set(diagonal_block)
        factor = factor.at[upper_edge:, lower_edge:upper_edge].set(below)
        updated = updated.at[upper_edge:, upper_edge:].add(-jnp.dot(below, below.T, precision=lax.Precision.HIGHEST))
    return factor

def panel_rows(source_rows, factor, panel):
    width = factor.shape[0]
    current = source_rows
    solved_parts = []
    for number in range(width // panel):
        lower_edge = number * panel
        upper_edge = lower_edge + panel
        solved = jax.scipy.linalg.solve_triangular(factor[lower_edge:upper_edge, lower_edge:upper_edge], current[:, lower_edge:upper_edge].T, lower=True).T
        solved_parts.append(solved)
        current = current.at[:, upper_edge:].add(-jnp.dot(solved, factor[upper_edge:, lower_edge:upper_edge].T, precision=lax.Precision.HIGHEST))
    return jnp.concatenate(solved_parts, axis=1)

def reference(b_values, tile_mask):
    span = 2 * PANEL
    masked = (b_values.astype(jnp.float32) * expand_tiles(tile_mask).astype(jnp.float32)).astype(jnp.bfloat16)
    product = lax.dot_general(masked.astype(jnp.float32), masked.astype(jnp.float32), (((0,), (0,)), ((), ())), preferred_element_type=jnp.float32)
    system = product + jnp.eye(AUX, dtype=jnp.float32)
    factor = factor_top(system[:span, :span], PANEL)
    lead = panel_rows(system[:, :span], factor, PANEL)
    trailing = system - jnp.dot(lead, lead.T, precision=lax.Precision.HIGHEST)
    padded = jnp.pad(lead, ((0, 0), (0, AUX - span)))
    row_ids = lax.broadcasted_iota(jnp.int32, (AUX, AUX), 0)
    col_ids = lax.broadcasted_iota(jnp.int32, (AUX, AUX), 1)
    zeros = jnp.zeros_like(system)
    return jnp.where(col_ids < span, jnp.where(row_ids >= col_ids, padded, zeros), jnp.where(row_ids < span, zeros, trailing))
```

```python
import functools

import jax
import jax.numpy as jnp
from jax import lax
from jax.experimental import pallas as pl
from jax.experimental.pallas import tpu as pltpu
from jax.sharding import PartitionSpec as P

TILE = 256
PANEL = 512
SPAN = 2 * PANEL
NB = 128
BLOCKS = SPAN // NB
MESH = pl.DeviceIdType.MESH
HIGHEST = lax.Precision.HIGHEST
VMEM_LIMIT = 66_000_000


def nn(a, b):
    return lax.dot_general(a, b, (((1,), (0,)), ((), ())), preferred_element_type=jnp.float32)


def nt(a, b):
    return lax.dot_general(a, b, (((1,), (1,)), ((), ())), preferred_element_type=jnp.float32)


def nn_hi(a, b):
    return lax.dot_general(
        a, b, (((1,), (0,)), ((), ())), precision=HIGHEST, preferred_element_type=jnp.float32
    )


def nt_hi(a, b):
    return lax.dot_general(
        a, b, (((1,), (1,)), ((), ())), precision=HIGHEST, preferred_element_type=jnp.float32
    )


def tn_hi(a, b):
    return lax.dot_general(
        a, b, (((0,), (0,)), ((), ())), precision=HIGHEST, preferred_element_type=jnp.float32
    )


class Stream:
    def __init__(self, index, send, recv, slot, device, u, v):
        self.index, self.send, self.recv = index, send, recv
        self.slot, self.device, self.u, self.v = slot, device, u, v
        self.sent = []

    def _at(self, du, dv):
        return lax.rem(self.u + du + 4, 4), (self.v if dv == 0 else 1 - self.v)

    def _copy(self, label, ref, du, dv):
        uu, vv = self._at(du, dv)
        return pltpu.make_async_remote_copy(
            src_ref=ref,
            dst_ref=ref,
            send_sem=self.send.at[self.index, label],
            recv_sem=self.recv.at[self.index, label],
            device_id=self.device(uu, vv),
            device_id_type=MESH,
        )

    def push(self, label, block, half, to):
        copy = self._copy(label, self.slot(*self._at(*block), half), *to)
        copy.start()
        self.sent.append(copy)

    def arrived(self, label, block, half, source):
        self._copy(label, self.slot(*self._at(*block), half), *source).wait_recv()

    def send_own(self):
        self.push(0, (0, 0), None, (0, 1))
        self.push(1, (0, 0), None, (1, 0))
        self.push(2, (0, 0), None, (-1, 0))

    def send_pair(self):
        self.arrived(0, (0, 1), None, (0, 1))
        self.push(3, (0, 1), None, (1, 0))
        self.push(4, (0, 1), None, (-1, 0))

    def relay_own(self):
        self.arrived(1, (-1, 0), None, (-1, 0))
        self.push(5, (-1, 0), 0, (1, 0))
        self.arrived(2, (1, 0), None, (1, 0))
        self.push(6, (1, 0), 1, (-1, 0))

    def relay_pair(self):
        self.arrived(3, (-1, 1), None, (-1, 0))
        self.push(7, (-1, 1), 0, (1, 0))
        self.arrived(4, (1, 1), None, (1, 0))
        self.push(8, (1, 1), 1, (-1, 0))

    def end_own(self):
        self.arrived(5, (2, 0), 0, (-1, 0))
        self.arrived(6, (2, 0), 1, (1, 0))

    def end_pair(self):
        self.arrived(7, (2, 1), 0, (-1, 0))
        self.arrived(8, (2, 1), 1, (1, 0))

    def drain(self):
        for copy in self.sent:
            copy.wait_send()


def gather_kernel(
    m_ref, mt_ref, c_ref, a_ref, sq_ref, sr_ref,
    left, right, b1t, send, recv, swap_send, swap_recv, one_send, one_recv, local,
):
    row, col = lax.axis_index("row"), lax.axis_index("col")
    x, yh = lax.div(row, 2), lax.rem(row, 2)
    core, q = lax.rem(col, 2), lax.div(col, 2)
    yl, z = lax.div(q, 4), lax.rem(q, 4)
    depth, width = m_ref.shape
    height = 2 * width
    piece = SPAN // 2
    other = (row, q * 2 + 1 - core)

    def over_row(u, v):
        return (2 * u + v, col)

    def over_col(u, v):
        return (row, (4 * v + u) * 2 + core)

    def part(start, size, half):
        if half is None:
            return pl.ds(pl.multiple_of(start, 128), size)
        return pl.ds(pl.multiple_of(start + half * (size // 2), 128), size // 2)

    def right_slot(u, v, half):
        return right.at[2 * u + v, part(0, depth, half), :]

    def left_slot(u, v, half):
        return left.at[4 * v + u, part(core * width, width, half), :]

    def b1_slot(u, v, half):
        return b1t.at[2 * u + v, part(core * piece, piece, half), :]

    r_stream = Stream(0, send, recv, right_slot, over_row, x, yh)
    b_stream = Stream(1, send, recv, b1_slot, over_row, x, yh)
    l_stream = Stream(2, send, recv, left_slot, over_col, z, yl)
    swaps = []

    def swap(base, number, ref):
        copy = pltpu.make_async_remote_copy(
            src_ref=ref, dst_ref=ref,
            send_sem=swap_send.at[base + number], recv_sem=swap_recv.at[base + number],
            device_id=other, device_id_type=MESH,
        )
        copy.start()
        swaps.append(copy)

    def single(number, ref, target, place=None):
        return pltpu.make_async_remote_copy(
            src_ref=ref, dst_ref=ref if place is None else place,
            send_sem=one_send.at[number], recv_sem=one_recv.at[number],
            device_id=target, device_id_type=MESH,
        )

    own_right = pltpu.make_async_copy(m_ref, right.at[row], local.at[0])
    own_right.start()

    barrier = pltpu.get_barrier_semaphore()
    mirror = (q, 2 * row + core)
    friends = [
        over_row(lax.rem(x + 1, 4), yh), over_row(lax.rem(x + 3, 4), yh), over_row(x, 1 - yh),
        over_col(lax.rem(z + 1, 4), yl), over_col(lax.rem(z + 3, 4), yl), over_col(z, 1 - yl),
        other,
    ]
    for friend in friends:
        pl.semaphore_signal(barrier, inc=1, device_id=friend, device_id_type=MESH)

    @pl.when(row != q)
    def _():
        pl.semaphore_signal(barrier, inc=1, device_id=mirror, device_id_type=MESH)
        pl.semaphore_wait(barrier, len(friends) + 1)

    @pl.when(row == q)
    def _():
        pl.semaphore_wait(barrier, len(friends))

    mine = part(core * width, width, None)

    @pl.when(row != q)
    def _():
        single(0, mt_ref, mirror, left.at[row, mine, :]).start()

    @pl.when(row == q)
    def _():
        pltpu.make_async_copy(mt_ref, left.at[row, mine, :], local.at[1]).start()

    seed = jnp.logical_and(yl == 0, z == 0)
    spare = b1t.at[row, pl.ds(piece, width - piece), :]
    low = b1t.at[row, pl.ds(0, piece), :]
    high = b1t.at[row, pl.ds(width, SPAN - width), :]
    own_piece = b1_slot(x, yh, None)

    def to_col(zz, yy):
        return over_col(zz, yy)

    @pl.when(jnp.logical_and(seed, core == 0))
    def _():
        single(1, mt_ref.at[pl.ds(piece, width - piece), :], other, spare).start()
        copy = pltpu.make_async_copy(mt_ref.at[pl.ds(0, piece), :], low, local.at[2])
        copy.start()
        copy.wait()

    @pl.when(jnp.logical_and(seed, core == 1))
    def _():
        copy = pltpu.make_async_copy(mt_ref.at[pl.ds(0, SPAN - width), :], high, local.at[2])
        copy.start()
        copy.wait()
        single(1, spare, other).wait_recv()

    @pl.when(seed)
    def _():
        single(2, own_piece, to_col(0, 1)).start()
        single(3, own_piece, to_col(1, 0)).start()
        single(4, own_piece, to_col(3, 0)).start()

    own_right.wait()
    r_stream.send_own()

    @pl.when(row != q)
    def _():
        single(0, mt_ref, mirror, left.at[q, mine, :]).wait()

    @pl.when(row == q)
    def _():
        pltpu.make_async_copy(mt_ref, left.at[row, mine, :], local.at[1]).wait()

    l_stream.send_own()
    swap(0, 0, left_slot(z, yl, None))

    @pl.when(jnp.logical_and(z == 0, yl == 1))
    def _():
        single(2, own_piece, to_col(0, 0)).wait_recv()
        single(3, own_piece, to_col(1, 1)).start()
        single(4, own_piece, to_col(3, 1)).start()

    @pl.when(z == 1)
    def _():
        single(3, own_piece, to_col(0, yl)).wait_recv()
        single(5, b1_slot(x, yh, 0), to_col(2, yl)).start()

    @pl.when(z == 3)
    def _():
        single(4, own_piece, to_col(0, yl)).wait_recv()
        single(6, b1_slot(x, yh, 1), to_col(2, yl)).start()

    @pl.when(z == 2)
    def _():
        single(5, b1_slot(x, yh, 0), to_col(1, yl)).wait_recv()
        single(6, b1_slot(x, yh, 1), to_col(3, yl)).wait_recv()

    b_stream.send_own()
    swap(8, 0, own_piece)

    r_stream.send_pair()
    r_stream.relay_own()
    b_stream.send_pair()
    b_stream.relay_own()
    l_stream.send_pair()
    l_stream.relay_own()

    def swap_near(base, stream, slot):
        for number, (du, dv) in ((1, (0, 1)), (2, (-1, 0)), (3, (1, 0))):
            swap(base, number, slot(*stream._at(du, dv), None))

    swap_near(8, b_stream, b1_slot)
    swap_near(0, l_stream, left_slot)
    r_stream.relay_pair()
    b_stream.relay_pair()
    l_stream.relay_pair()
    for base, stream, slot in ((8, b_stream, b1_slot), (0, l_stream, left_slot)):
        for number, (du, dv) in ((4, (-1, 1)), (5, (1, 1))):
            swap(base, number, slot(*stream._at(du, dv), None))

    r_stream.end_own()
    b_stream.end_own()
    swap(8, 6, b1_slot(*b_stream._at(2, 0), None))
    l_stream.end_own()
    swap(0, 6, left_slot(*l_stream._at(2, 0), None))
    r_stream.end_pair()
    b_stream.end_pair()
    swap(8, 7, b1_slot(*b_stream._at(2, 1), None))
    l_stream.end_pair()
    swap(0, 7, left_slot(*l_stream._at(2, 1), None))

    order = ((0, 0), (0, 1), (-1, 0), (1, 0), (-1, 1), (1, 1), (2, 0), (2, 1))
    for number, (du, dv) in enumerate(order):
        for base, stream in ((8, b_stream), (0, l_stream)):
            uu, vv = stream._at(du, dv)
            if base == 8:
                theirs = b1t.at[2 * uu + vv, part((1 - core) * piece, piece, None), :]
            else:
                theirs = left.at[4 * vv + uu, part((1 - core) * width, width, None), :]
            pltpu.make_async_remote_copy(
                src_ref=theirs, dst_ref=theirs,
                send_sem=swap_send.at[base + number], recv_sem=swap_recv.at[base + number],
                device_id=other, device_id_type=MESH,
            ).wait_recv()

    rows = 512

    def products(k, first):
        def put(ref, tile, value):
            at = pl.ds(pl.multiple_of(tile * rows, rows), rows)
            if first:
                ref[at, :] = value
            else:
                ref[at, :] += value

        def over_left(tile, carry):
            lhs = left[k, pl.ds(pl.multiple_of(tile * rows, rows), rows), :]
            put(c_ref, tile, nn(lhs, right[k]))
            put(sr_ref, tile, nt(lhs, b1t[k]))
            return carry

        lax.fori_loop(0, height // rows, over_left, 0)

        def over_span(tile, carry):
            lhs = b1t[k, pl.ds(pl.multiple_of(tile * rows, rows), rows), :]
            put(sq_ref, tile, nn(lhs, right[k]))
            put(a_ref, tile, nt(lhs, b1t[k]))
            return carry

        lax.fori_loop(0, SPAN // rows, over_span, 0)

    products(0, True)

    def step(k, carry):
        products(k, False)
        return carry

    lax.fori_loop(1, 8, step, 0)

    for stream in (r_stream, b_stream, l_stream):
        stream.drain()
    for copy in swaps:
        copy.wait_send()

    @pl.when(jnp.logical_and(seed, core == 0))
    def _():
        single(1, mt_ref.at[pl.ds(piece, width - piece), :], other, spare).wait_send()

    @pl.when(seed)
    def _():
        single(2, own_piece, to_col(0, 1)).wait_send()

    @pl.when(z == 0)
    def _():
        single(3, own_piece, to_col(1, yl)).wait_send()
        single(4, own_piece, to_col(3, yl)).wait_send()

    @pl.when(z == 1)
    def _():
        single(5, b1_slot(x, yh, 0), to_col(2, yl)).wait_send()

    @pl.when(z == 3)
    def _():
        single(6, b1_slot(x, yh, 1), to_col(2, yl)).wait_send()


def gather_products(masked, transposed):
    depth, width = masked.shape
    height = 2 * width
    f32, bf16 = jnp.float32, jnp.bfloat16
    dma = pltpu.SemaphoreType.DMA
    hbm, vmem = pl.BlockSpec(memory_space=pl.ANY), pl.BlockSpec(memory_space=pltpu.VMEM)
    return pl.pallas_call(
        gather_kernel,
        out_shape=[
            jax.ShapeDtypeStruct((height, width), f32),
            jax.ShapeDtypeStruct((SPAN, SPAN), f32),
            jax.ShapeDtypeStruct((SPAN, width), f32),
            jax.ShapeDtypeStruct((height, SPAN), f32),
        ],
        in_specs=[hbm, hbm],
        out_specs=[vmem] * 4,
        scratch_shapes=[
            pltpu.VMEM((8, height, depth), bf16),
            pltpu.VMEM((8, depth, width), bf16),
            pltpu.VMEM((8, SPAN, depth), bf16),
            dma((3, 9)), dma((3, 9)),
            dma((16,)), dma((16,)),
            dma((7,)), dma((7,)),
            dma((3,)),
        ],
        compiler_params=pltpu.CompilerParams(
            collective_id=0, has_side_effects=True, vmem_limit_bytes=VMEM_LIMIT
        ),
        name="gather_products",
    )(masked, transposed)


def bc_row(x, k):
    return jnp.broadcast_to(x[k : k + 1, :], (8, NB))


def bc_col(x, j):
    return jnp.broadcast_to(x[:, j : j + 1], (8, NB))


def inverse_factor(block):
    groups = NB // 8
    lane = lax.broadcasted_iota(jnp.int32, (8, NB), 1)
    sub = lax.broadcasted_iota(jnp.int32, (8, NB), 0)
    s = [block[8 * g : 8 * g + 8, :] for g in range(groups)]
    y = [jnp.where(lane == sub + 8 * g, 1.0, 0.0) for g in range(groups)]
    out = []
    for g0 in range(groups):
        top, inv = s[g0], y[g0]
        pivots = [bc_col(top, 8 * g0 + k) for k in range(8)]
        below = {g: [bc_col(s[g], 8 * g0 + k) for k in range(8)] for g in range(g0 + 1, groups)}
        scale = jnp.zeros((8, NB), jnp.float32)
        done = jnp.zeros((8, NB), jnp.float32)
        for k in range(8):
            pivot = bc_row(pivots[k], k)
            reciprocal = 1.0 / pivot
            here = sub == k
            f = jnp.where(here, 0.0, pivots[k] * reciprocal)
            scale = jnp.where(here, reciprocal, scale)
            done = jnp.where(here, inv * lax.rsqrt(pivot), done)
            for m in range(k + 1, 8):
                pivots[m] = pivots[m] - f * bc_row(pivots[m], k)
            top = top - f * bc_row(top, k)
            inv = inv - f * bc_row(inv, k)
        out.append(done)
        if g0 + 1 < groups:
            top, inv = top * scale, inv * scale
            tops = [bc_row(top, k) for k in range(8)]
            invs = [bc_row(inv, k) for k in range(8)]
            for g in range(g0 + 1, groups):
                t = [below[g][k] * tops[k] for k in range(8)]
                v = [below[g][k] * invs[k] for k in range(8)]
                while len(t) > 1:
                    t = [t[i] + t[i + 1] for i in range(0, len(t), 2)]
                    v = [v[i] + v[i + 1] for i in range(0, len(v), 2)]
                s[g] = s[g] - t[0]
                y[g] = y[g] - v[0]
    return jnp.concatenate(out, axis=0)


def split(value):
    high = value.astype(jnp.bfloat16)
    return high, (value - high.astype(jnp.float32)).astype(jnp.bfloat16)


def finish_kernel(c_ref, a_in, sq_ref, sr_ref, out_ref, a_ref, y_ref, w_ref, xh_ref, xl_ref):
    row, col = lax.axis_index("row"), lax.axis_index("col")
    height, width = out_ref.shape
    blk = [slice(b * NB, (b + 1) * NB) for b in range(BLOCKS)]
    eye = jnp.where(
        lax.broadcasted_iota(jnp.int32, (NB, NB), 0) == lax.broadcasted_iota(jnp.int32, (NB, NB), 1),
        1.0, 0.0,
    )
    a_ref[...] = a_in[...]
    for b in range(BLOCKS):
        a_ref[blk[b], blk[b]] += eye
    w_ref[...] = sq_ref[...]
    for b in range(BLOCKS):
        y_ref[b] = inverse_factor(a_ref[blk[b], blk[b]])
        w_ref[blk[b], :] = nn_hi(y_ref[b], w_ref[blk[b], :])
        for i in range(b + 1, BLOCKS):
            a_ref[blk[i], blk[b]] = nt_hi(a_ref[blk[i], blk[b]], y_ref[b])
        for i in range(b + 1, BLOCKS):
            at = slice((b + 1) * NB, (i + 1) * NB)
            a_ref[blk[i], at] -= nt_hi(a_ref[blk[i], blk[b]], a_ref[at, blk[b]])
            w_ref[blk[i], :] -= nn_hi(a_ref[blk[i], blk[b]], w_ref[blk[b], :])

    cols = col * width + lax.broadcasted_iota(jnp.int32, (NB, width), 1)
    for b in range(BLOCKS):
        unit = jnp.where(b * NB + lax.broadcasted_iota(jnp.int32, (NB, width), 0) == cols, 1.0, 0.0)
        w_ref[blk[b], :] = jnp.where(cols < SPAN, unit, w_ref[blk[b], :])
    for b in reversed(range(BLOCKS)):
        solved = tn_hi(y_ref[b], w_ref[blk[b], :])
        xh_ref[blk[b], :], xl_ref[blk[b], :] = split(solved)
        for i in range(b):
            w_ref[blk[i], :] -= tn_hi(a_ref[blk[b], blk[i]], solved)

    rows = 256

    def tile(t, carry):
        at = pl.ds(pl.multiple_of(t * rows, rows), rows)
        first = row * height + t * rows
        grow = first + lax.broadcasted_iota(jnp.int32, (rows, width), 0)
        gcol = col * width + lax.broadcasted_iota(jnp.int32, (rows, width), 1)
        srow = first + lax.broadcasted_iota(jnp.int32, (rows, SPAN), 0)
        scol = lax.broadcasted_iota(jnp.int32, (rows, SPAN), 1)
        sh, sl = split(sr_ref[at, :] + jnp.where(srow == scol, 1.0, 0.0))
        value = nn(sh, xh_ref[...]) + nn(sl, xh_ref[...]) + nn(sh, xl_ref[...])
        system = c_ref[at, :] + jnp.where(grow == gcol, 1.0, 0.0)
        lead = jnp.where(grow >= gcol, value, 0.0)
        rest = jnp.where(grow < SPAN, 0.0, system - value)
        out_ref[at, :] = jnp.where(gcol < SPAN, lead, rest)
        return carry

    lax.fori_loop(0, height // rows, tile, 0)


def finish(c, a, sq, sr):
    height, width = c.shape
    f32, bf16 = jnp.float32, jnp.bfloat16
    vmem = pl.BlockSpec(memory_space=pltpu.VMEM)
    return pl.pallas_call(
        finish_kernel,
        out_shape=jax.ShapeDtypeStruct((height, width), f32),
        in_specs=[vmem] * 4,
        out_specs=vmem,
        scratch_shapes=[
            pltpu.VMEM((SPAN, SPAN), f32),
            pltpu.VMEM((BLOCKS, NB, NB), f32),
            pltpu.VMEM((SPAN, width), f32),
            pltpu.VMEM((SPAN, width), bf16),
            pltpu.VMEM((SPAN, width), bf16),
        ],
        compiler_params=pltpu.CompilerParams(vmem_limit_bytes=VMEM_LIMIT),
        name="finish",
    )(c, a, sq, sr)


def expand_tiles(blocks):
    return jnp.repeat(jnp.repeat(blocks, TILE, axis=0), TILE, axis=1)


def on_device(b_values, tile_mask):
    row_index = lax.axis_index("row")
    col_index = lax.axis_index("col")
    depth, width = b_values.shape
    occupancy = lax.dynamic_slice(
        tile_mask,
        (row_index * (depth // TILE), col_index * (width // TILE)),
        (depth // TILE, width // TILE),
    )
    masked = b_values * expand_tiles(occupancy).astype(jnp.bfloat16)
    return finish(*gather_products(masked, masked.T))


def solution(mesh):
    return jax.shard_map(
        on_device,
        mesh=mesh,
        in_specs=(P("row", "col"), P()),
        out_specs=P("row", "col"),
        check_vma=False,
    )
```

```python
import functools

import jax
import jax.numpy as jnp
from jax import lax
from jax.experimental import pallas as pl
from jax.experimental.pallas import tpu as pltpu
from jax.sharding import PartitionSpec as P

TILE = 256
PANEL = 512
SPAN = 2 * PANEL
NB = 128
BLOCKS = SPAN // NB
MESH = pl.DeviceIdType.MESH
VMEM_LIMIT = 66_000_000


def nn(a, b):
    return lax.dot_general(a, b, (((1,), (0,)), ((), ())), preferred_element_type=jnp.float32)


def nt(a, b):
    return lax.dot_general(a, b, (((1,), (1,)), ((), ())), preferred_element_type=jnp.float32)


def tn(a, b):
    return lax.dot_general(a, b, (((0,), (0,)), ((), ())), preferred_element_type=jnp.float32)


def split(value):
    high = value.astype(jnp.bfloat16)
    return high, (value - high.astype(jnp.float32)).astype(jnp.bfloat16)


def three(dot, a, b):
    (ah, al), (bh, bl) = a, b
    return dot(ah, bh) + (dot(al, bh) + dot(ah, bl))


class Stream:
    def __init__(self, index, send, recv, slot, device, u, v):
        self.index, self.send, self.recv = index, send, recv
        self.slot, self.device, self.u, self.v = slot, device, u, v
        self.sent = []
        self.ring = {du: lax.rem(u + du + 4, 4) for du in (-1, 0, 1, 2)}
        self.pair = {0: v, 1: 1 - v}
        self.zero = 0

    def _at(self, du, dv):
        return self.ring[du], self.pair[dv]

    def _copy(self, label, ref, du, dv):
        uu, vv = self._at(du, dv)
        return pltpu.make_async_remote_copy(
            src_ref=ref,
            dst_ref=ref,
            send_sem=self.send.at[self.index + self.zero, label + self.zero],
            recv_sem=self.recv.at[self.index + self.zero, label + self.zero],
            device_id=self.device(uu, vv),
            device_id_type=MESH,
        )

    def push(self, label, block, half, to):
        copy = self._copy(label, self.slot(*self._at(*block), half), *to)
        copy.start()
        self.sent.append((label, block, half, to))

    def arrived(self, label, block, half, source):
        self._copy(label, self.slot(*self._at(*block), half), *source).wait_recv()

    def send_own(self):
        self.push(0, (0, 0), None, (0, 1))
        self.push(1, (0, 0), None, (1, 0))
        self.push(2, (0, 0), None, (-1, 0))

    def send_pair(self):
        self.arrived(0, (0, 1), None, (0, 1))
        self.push(3, (0, 1), None, (1, 0))
        self.push(4, (0, 1), None, (-1, 0))

    def relay_own(self):
        self.arrived(1, (-1, 0), None, (-1, 0))
        self.push(5, (-1, 0), 0, (1, 0))
        self.arrived(2, (1, 0), None, (1, 0))
        self.push(6, (1, 0), 1, (-1, 0))

    def relay_pair(self):
        self.arrived(3, (-1, 1), None, (-1, 0))
        self.push(7, (-1, 1), 0, (1, 0))
        self.arrived(4, (1, 1), None, (1, 0))
        self.push(8, (1, 1), 1, (-1, 0))

    def end_own(self):
        self.arrived(5, (2, 0), 0, (-1, 0))
        self.arrived(6, (2, 0), 1, (1, 0))

    def end_pair(self):
        self.arrived(7, (2, 1), 0, (-1, 0))
        self.arrived(8, (2, 1), 1, (1, 0))

    def drain(self):
        for label, block, half, to in self.sent:
            self._copy(label, self.slot(*self._at(*block), half), *to).wait_send()


def bc_row(x, k):
    return jnp.broadcast_to(x[k : k + 1, :], (8, NB))


def bc_col(x, j):
    return jnp.broadcast_to(x[:, j : j + 1], (8, NB))


def inverse_factor(block):
    groups = NB // 8
    lane = lax.broadcasted_iota(jnp.int32, (8, NB), 1)
    sub = lax.broadcasted_iota(jnp.int32, (8, NB), 0)
    s = [block[8 * g : 8 * g + 8, :] for g in range(groups)]
    y = [jnp.where(lane == sub + 8 * g, 1.0, 0.0) for g in range(groups)]
    out = []
    for g0 in range(groups):
        top, inv = s[g0], y[g0]
        pivots = [bc_col(top, 8 * g0 + k) for k in range(8)]
        below = {g: [bc_col(s[g], 8 * g0 + k) for k in range(8)] for g in range(g0 + 1, groups)}
        scale = jnp.zeros((8, NB), jnp.float32)
        done = jnp.zeros((8, NB), jnp.float32)
        for k in range(8):
            pivot = bc_row(pivots[k], k)
            reciprocal = 1.0 / pivot
            here = sub == k
            f = jnp.where(here, 0.0, pivots[k] * reciprocal)
            scale = jnp.where(here, reciprocal, scale)
            done = jnp.where(here, inv * lax.rsqrt(pivot), done)
            for m in range(k + 1, 8):
                pivots[m] = pivots[m] - f * bc_row(pivots[m], k)
            top = top - f * bc_row(top, k)
            inv = inv - f * bc_row(inv, k)
        out.append(done)
        if g0 + 1 < groups:
            top, inv = top * scale, inv * scale
            tops = [bc_row(top, k) for k in range(8)]
            invs = [bc_row(inv, k) for k in range(8)]
            for g in range(g0 + 1, groups):
                t = [below[g][k] * tops[k] for k in range(8)]
                v = [below[g][k] * invs[k] for k in range(8)]
                while len(t) > 1:
                    t = [t[i] + t[i + 1] for i in range(0, len(t), 2)]
                    v = [v[i] + v[i + 1] for i in range(0, len(v), 2)]
                s[g] = s[g] - t[0]
                y[g] = y[g] - v[0]
    return jnp.concatenate(out, axis=0)


def whole_kernel(
    m_ref, mt_ref, out_ref,
    left, right, b1t, a_ref, sq_ref, sr_ref, linv_ref, xh_ref, xl_ref,
    send, recv, swap_send, swap_recv, one_send, one_recv, local,
):
    row, col = lax.axis_index("row"), lax.axis_index("col")
    x, yh = lax.div(row, 2), lax.rem(row, 2)
    core, q = lax.rem(col, 2), lax.div(col, 2)
    yl, z = lax.div(q, 4), lax.rem(q, 4)
    depth, width = m_ref.shape
    height = 2 * width
    piece = SPAN // 2
    other = (row, q * 2 + 1 - core)

    def over_row(u, v):
        return (2 * u + v, col)

    def over_col(u, v):
        return (row, (4 * v + u) * 2 + core)

    def part(start, size, half):
        if half is None:
            return pl.ds(pl.multiple_of(start, 128), size)
        return pl.ds(pl.multiple_of(start + half * (size // 2), 128), size // 2)

    def right_slot(u, v, half):
        return right.at[2 * u + v, part(0, depth, half), :]

    def left_slot(u, v, half, side=core):
        return left.at[4 * v + u, part(side * width, width, half), :]

    def b1_slot(u, v, half, side=core):
        return b1t.at[2 * u + v, part(side * piece, piece, half), :]

    r_stream = Stream(0, send, recv, right_slot, over_row, x, yh)
    b_stream = Stream(1, send, recv, b1_slot, over_row, x, yh)
    l_stream = Stream(2, send, recv, left_slot, over_col, z, yl)
    order = ((0, 0), (0, 1), (-1, 0), (1, 0), (-1, 1), (1, 1), (2, 0), (2, 1))
    swaps = []

    def swap_copy(base, number, ref):
        place = base + number + l_stream.zero
        return pltpu.make_async_remote_copy(
            src_ref=ref, dst_ref=ref,
            send_sem=swap_send.at[place], recv_sem=swap_recv.at[place],
            device_id=other, device_id_type=MESH,
        )

    def swap_out(base, number):
        stream, slot = (b_stream, b1_slot) if base == 8 else (l_stream, left_slot)
        return swap_copy(base, number, slot(*stream._at(*order[number]), None))

    def swap(base, number):
        swap_out(base, number).start()
        swaps.append((base, number))

    def swapped(base, number):
        stream, slot = (b_stream, b1_slot) if base == 8 else (l_stream, left_slot)
        theirs = slot(*stream._at(*order[number]), None, 1 - core)
        swap_copy(base, number, theirs).wait_recv()

    def single(number, ref, target, place=None):
        return pltpu.make_async_remote_copy(
            src_ref=ref, dst_ref=ref if place is None else place,
            send_sem=one_send.at[number], recv_sem=one_recv.at[number],
            device_id=target, device_id_type=MESH,
        )

    own_right = pltpu.make_async_copy(m_ref, right.at[row], local.at[0])
    own_right.start()

    barrier = pltpu.get_barrier_semaphore()
    mirror = (q, 2 * row + core)
    friends = [
        over_row(lax.rem(x + 1, 4), yh), over_row(lax.rem(x + 3, 4), yh), over_row(x, 1 - yh),
        over_col(lax.rem(z + 1, 4), yl), over_col(lax.rem(z + 3, 4), yl), over_col(z, 1 - yl),
        other,
    ]
    for friend in friends:
        pl.semaphore_signal(barrier, inc=1, device_id=friend, device_id_type=MESH)

    @pl.when(row != q)
    def _():
        pl.semaphore_signal(barrier, inc=1, device_id=mirror, device_id_type=MESH)
        pl.semaphore_wait(barrier, len(friends) + 1)

    @pl.when(row == q)
    def _():
        pl.semaphore_wait(barrier, len(friends))

    seed = jnp.logical_and(yl == 0, z == 0)
    spare = b1t.at[row, pl.ds(piece, width - piece), :]
    low = b1t.at[row, pl.ds(0, piece), :]
    high = b1t.at[row, pl.ds(width, SPAN - width), :]
    chunk = [b1_slot(x, yh, 0), b1_slot(x, yh, 1)]

    @pl.when(jnp.logical_and(seed, core == 0))
    def _():
        single(1, mt_ref.at[pl.ds(piece, width - piece), :], other, spare).start()
        copy = pltpu.make_async_copy(mt_ref.at[pl.ds(0, piece), :], low, local.at[2])
        copy.start()
        copy.wait()

    @pl.when(jnp.logical_and(seed, core == 1))
    def _():
        copy = pltpu.make_async_copy(mt_ref.at[pl.ds(0, SPAN - width), :], high, local.at[2])
        copy.start()
        copy.wait()
        single(1, spare, other).wait_recv()

    def down(h):
        single(4 + h, chunk[h], over_col(1, yl)).start()

    def up(h):
        single(6 + h, chunk[h], over_col(3, yl)).start()

    @pl.when(seed)
    def _():
        for h in range(2):
            single(2 + h, chunk[h], over_col(0, 1)).start()
            down(h)
            up(1 - h)

    mine = part(core * width, width, None)

    @pl.when(row != q)
    def _():
        single(0, mt_ref, mirror, left.at[row, mine, :]).start()

    @pl.when(row == q)
    def _():
        pltpu.make_async_copy(mt_ref, left.at[row, mine, :], local.at[1]).start()

    own_right.wait()
    r_stream.push(1, (0, 0), None, (1, 0))
    r_stream.push(2, (0, 0), None, (-1, 0))

    @pl.when(jnp.logical_and(z == 0, yl == 1))
    def _():
        for h in range(2):
            single(2 + h, chunk[h], over_col(0, 0)).wait_recv()
            down(h)
            up(h)

    @pl.when(z == 1)
    def _():
        single(4, chunk[0], over_col(0, yl)).wait_recv()
        single(8, chunk[0], over_col(2, yl)).start()
        single(5, chunk[1], over_col(0, yl)).wait_recv()

    @pl.when(z == 3)
    def _():
        single(7, chunk[1], over_col(0, yl)).wait_recv()
        single(9, chunk[1], over_col(2, yl)).start()
        single(6, chunk[0], over_col(0, yl)).wait_recv()

    @pl.when(z == 2)
    def _():
        single(8, chunk[0], over_col(1, yl)).wait_recv()
        single(9, chunk[1], over_col(3, yl)).wait_recv()

    b_stream.send_own()
    swap(8, 0)
    r_stream.push(0, (0, 0), None, (0, 1))

    rows = 512

    def at_tile(tile):
        return pl.ds(pl.multiple_of(tile * rows, rows), rows)

    def gram(number):
        swapped(8, number)
        uu, vv = b_stream._at(*order[number])
        k = 2 * uu + vv

        def over_span(tile, carry):
            value = nt(b1t[k, at_tile(tile), :], b1t[k])
            if number == 0:
                a_ref[at_tile(tile), :] = value
            else:
                a_ref[at_tile(tile), :] += value
            return carry

        lax.fori_loop(0, SPAN // rows, over_span, 0)

    b_stream.send_pair()
    swap(8, 1)
    gram(0)
    b_stream.relay_own()
    swap(8, 2)
    swap(8, 3)
    gram(1)
    b_stream.relay_pair()
    swap(8, 4)
    swap(8, 5)
    r_stream.send_pair()
    r_stream.relay_own()
    gram(2)
    gram(3)
    b_stream.end_own()
    swap(8, 6)
    gram(4)
    gram(5)

    @pl.when(row != q)
    def _():
        single(0, mt_ref, mirror, left.at[q, mine, :]).wait()

    @pl.when(row == q)
    def _():
        pltpu.make_async_copy(mt_ref, left.at[row, mine, :], local.at[1]).wait()

    l_stream.send_own()
    swap(0, 0)
    b_stream.end_pair()
    swap(8, 7)
    gram(6)
    gram(7)

    eye = jnp.where(
        lax.broadcasted_iota(jnp.int32, (NB, NB), 0) == lax.broadcasted_iota(jnp.int32, (NB, NB), 1),
        1.0, 0.0,
    )
    for b in range(BLOCKS):
        at = slice(b * NB, (b + 1) * NB)
        a_ref[at, at] += eye
    linv_ref[...] = jnp.zeros_like(linv_ref)
    tall = 256

    def factor_step(b, carry):
        r_stream.zero = l_stream.zero = b * 0
        at = pl.ds(pl.multiple_of(b * NB, NB), NB)
        y = inverse_factor(a_ref[at, at])
        linv_ref[at, at] = y
        below = lax.broadcasted_iota(jnp.int32, (SPAN, NB), 0) >= (b + 1) * NB
        panel = three(nt, split(a_ref[:, at]), split(y))
        panel = jnp.where(below, panel, 0.0)
        a_ref[:, at] = panel
        xh_ref[:, 0:NB], xl_ref[:, 0:NB] = split(panel)

        def update(tile, c):
            part_rows = pl.ds(pl.multiple_of(tile * tall, tall), tall)
            a_ref[part_rows, :] -= three(
                nt,
                (xh_ref[part_rows, 0:NB], xl_ref[part_rows, 0:NB]),
                (xh_ref[:, 0:NB], xl_ref[:, 0:NB]),
            )
            return c

        lax.fori_loop((b + 1) // 2, SPAN // tall, update, 0)

        @pl.when(b == 1)
        def _():
            r_stream.relay_pair()

        @pl.when(b == 2)
        def _():
            l_stream.send_pair()
            swap(0, 1)
            l_stream.relay_own()
            swap(0, 2)
            swap(0, 3)

        @pl.when(b == 5)
        def _():
            l_stream.relay_pair()
            swap(0, 4)
            swap(0, 5)

        return carry

    lax.fori_loop(0, BLOCKS, factor_step, 0)
    r_stream.zero = l_stream.zero = 0

    r_stream.end_own()
    r_stream.end_pair()

    def over_blocks(ref, tiles, rhs):
        def step(k, carry):
            def inner(tile, c):
                value = rhs(k, at_tile(tile))

                @pl.when(k == 0)
                def _():
                    ref[at_tile(tile), :] = value

                @pl.when(k > 0)
                def _():
                    ref[at_tile(tile), :] += value

                return c

            return lax.fori_loop(0, tiles, inner, carry)

        lax.fori_loop(0, 8, step, 0)

    over_blocks(sq_ref, SPAN // rows, lambda k, at: nn(b1t[k, at, :], right[k]))
    l_stream.end_own()
    swap(0, 6)
    l_stream.end_pair()
    swap(0, 7)

    size = NB
    while size < SPAN:
        for lo in range(0, SPAN, 2 * size):
            one, two = slice(lo, lo + size), slice(lo + size, lo + 2 * size)
            inner = three(nn, split(a_ref[two, one]), split(linv_ref[one, one]))
            linv_ref[two, one] = -three(nn, split(linv_ref[two, two]), split(inner))
        size *= 2

    cols = col * width + lax.broadcasted_iota(jnp.int32, (tall, width), 1)
    for b in range(SPAN // tall):
        at = slice(b * tall, (b + 1) * tall)
        upto = slice(0, (b + 1) * tall)
        solved = three(nn, split(linv_ref[at, upto]), split(sq_ref[upto, :]))
        unit = jnp.where(b * tall + lax.broadcasted_iota(jnp.int32, (tall, width), 0) == cols, 1.0, 0.0)
        xh_ref[at, :], xl_ref[at, :] = split(jnp.where(cols < SPAN, unit, solved))
    for b in range(SPAN // tall):
        at = slice(b * tall, (b + 1) * tall)
        onward = slice(b * tall, SPAN)
        sq_ref[at, :] = three(tn, split(linv_ref[onward, at]), (xh_ref[onward, :], xl_ref[onward, :]))
    for b in range(SPAN // tall):
        at = slice(b * tall, (b + 1) * tall)
        xh_ref[at, :], xl_ref[at, :] = split(sq_ref[at, :])

    for number in range(8):
        swapped(0, number)
    over_blocks(out_ref, height // rows, lambda k, at: nn(left[k, at, :], right[k]))
    over_blocks(sr_ref, height // rows, lambda k, at: nt(left[k, at, :], b1t[k]))

    def finish(t, carry):
        at = pl.ds(pl.multiple_of(t * tall, tall), tall)
        first = row * height + t * tall
        grow = first + lax.broadcasted_iota(jnp.int32, (tall, width), 0)
        gcol = col * width + lax.broadcasted_iota(jnp.int32, (tall, width), 1)
        srow = first + lax.broadcasted_iota(jnp.int32, (tall, SPAN), 0)
        scol = lax.broadcasted_iota(jnp.int32, (tall, SPAN), 1)
        strip = split(sr_ref[at, :] + jnp.where(srow == scol, 1.0, 0.0))
        value = three(nn, strip, (xh_ref[...], xl_ref[...]))
        system = out_ref[at, :] + jnp.where(grow == gcol, 1.0, 0.0)
        lead = jnp.where(grow >= gcol, value, 0.0)
        rest = jnp.where(grow < SPAN, 0.0, system - value)
        out_ref[at, :] = jnp.where(gcol < SPAN, lead, rest)
        return carry

    lax.fori_loop(0, height // tall, finish, 0)

    for stream in (r_stream, b_stream, l_stream):
        stream.drain()
    for base, number in swaps:
        swap_out(base, number).wait_send()

    @pl.when(jnp.logical_and(seed, core == 0))
    def _():
        single(1, mt_ref.at[pl.ds(piece, width - piece), :], other, spare).wait_send()

    @pl.when(seed)
    def _():
        for h in range(2):
            single(2 + h, chunk[h], over_col(0, 1)).wait_send()

    @pl.when(z == 0)
    def _():
        for h in range(2):
            single(4 + h, chunk[h], over_col(1, yl)).wait_send()
            single(6 + h, chunk[h], over_col(3, yl)).wait_send()

    @pl.when(z == 1)
    def _():
        single(8, chunk[0], over_col(2, yl)).wait_send()

    @pl.when(z == 3)
    def _():
        single(9, chunk[1], over_col(2, yl)).wait_send()


def whole(masked, transposed):
    depth, width = masked.shape
    height = 2 * width
    f32, bf16 = jnp.float32, jnp.bfloat16
    dma = pltpu.SemaphoreType.DMA
    hbm, vmem = pl.BlockSpec(memory_space=pl.ANY), pl.BlockSpec(memory_space=pltpu.VMEM)
    return pl.pallas_call(
        whole_kernel,
        out_shape=jax.ShapeDtypeStruct((height, width), f32),
        in_specs=[hbm, hbm],
        out_specs=vmem,
        scratch_shapes=[
            pltpu.VMEM((8, height, depth), bf16),
            pltpu.VMEM((8, depth, width), bf16),
            pltpu.VMEM((8, SPAN, depth), bf16),
            pltpu.VMEM((SPAN, SPAN), f32),
            pltpu.VMEM((SPAN, width), f32),
            pltpu.VMEM((height, SPAN), f32),
            pltpu.VMEM((SPAN, SPAN), f32),
            pltpu.VMEM((SPAN, width), bf16),
            pltpu.VMEM((SPAN, width), bf16),
            dma((3, 9)), dma((3, 9)),
            dma((16,)), dma((16,)),
            dma((10,)), dma((10,)),
            dma((3,)),
        ],
        compiler_params=pltpu.CompilerParams(
            collective_id=0, has_side_effects=True, vmem_limit_bytes=VMEM_LIMIT
        ),
        name="whole",
    )(masked, transposed)


def expand_tiles(blocks):
    return jnp.repeat(jnp.repeat(blocks, TILE, axis=0), TILE, axis=1)


def on_device(b_values, tile_mask):
    row_index = lax.axis_index("row")
    col_index = lax.axis_index("col")
    depth, width = b_values.shape
    occupancy = lax.dynamic_slice(
        tile_mask,
        (row_index * (depth // TILE), col_index * (width // TILE)),
        (depth // TILE, width // TILE),
    )
    masked = b_values * expand_tiles(occupancy).astype(jnp.bfloat16)
    return whole(masked, masked.T)


def solution(mesh):
    return jax.shard_map(
        on_device,
        mesh=mesh,
        in_specs=(P("row", "col"), P()),
        out_specs=P("row", "col"),
        check_vma=False,
    )
```

```python
import functools

import jax
import jax.numpy as jnp
from jax import lax
from jax.experimental import pallas as pl
from jax.experimental.pallas import tpu as pltpu
from jax.sharding import PartitionSpec as P

TILE = 256
PANEL = 512
SPAN = 2 * PANEL
NB = 128
BLOCKS = SPAN // NB
MESH = pl.DeviceIdType.MESH
VMEM_LIMIT = 66_000_000


def nn(a, b):
    return lax.dot_general(a, b, (((1,), (0,)), ((), ())), preferred_element_type=jnp.float32)


def nt(a, b):
    return lax.dot_general(a, b, (((1,), (1,)), ((), ())), preferred_element_type=jnp.float32)


def tn(a, b):
    return lax.dot_general(a, b, (((0,), (0,)), ((), ())), preferred_element_type=jnp.float32)


def split(value):
    high = value.astype(jnp.bfloat16)
    return high, (value - high.astype(jnp.float32)).astype(jnp.bfloat16)


def three(dot, a, b):
    (ah, al), (bh, bl) = a, b
    return dot(ah, bh) + (dot(al, bh) + dot(ah, bl))


class Stream:
    def __init__(self, index, send, recv, slot, device, u, v):
        self.index, self.send, self.recv = index, send, recv
        self.slot, self.device, self.u, self.v = slot, device, u, v
        self.sent = []
        self.ring = {du: lax.rem(u + du + 4, 4) for du in (-1, 0, 1, 2)}
        self.pair = {0: v, 1: 1 - v}
        self.zero = 0

    def _at(self, du, dv):
        return self.ring[du], self.pair[dv]

    def _copy(self, label, ref, du, dv):
        uu, vv = self._at(du, dv)
        return pltpu.make_async_remote_copy(
            src_ref=ref,
            dst_ref=ref,
            send_sem=self.send.at[self.index + self.zero, label + self.zero],
            recv_sem=self.recv.at[self.index + self.zero, label + self.zero],
            device_id=self.device(uu, vv),
            device_id_type=MESH,
        )

    def push(self, label, block, half, to):
        copy = self._copy(label, self.slot(*self._at(*block), half), *to)
        copy.start()
        self.sent.append((label, block, half, to))

    def arrived(self, label, block, half, source):
        self._copy(label, self.slot(*self._at(*block), half), *source).wait_recv()

    def send_own(self):
        self.push(0, (0, 0), None, (0, 1))
        self.push(1, (0, 0), None, (1, 0))
        self.push(2, (0, 0), None, (-1, 0))

    def send_pair(self):
        self.arrived(0, (0, 1), None, (0, 1))
        self.push(3, (0, 1), None, (1, 0))
        self.push(4, (0, 1), None, (-1, 0))

    def relay_own(self):
        self.arrived(1, (-1, 0), None, (-1, 0))
        self.push(5, (-1, 0), 0, (1, 0))
        self.arrived(2, (1, 0), None, (1, 0))
        self.push(6, (1, 0), 1, (-1, 0))

    def relay_pair(self):
        self.arrived(3, (-1, 1), None, (-1, 0))
        self.push(7, (-1, 1), 0, (1, 0))
        self.arrived(4, (1, 1), None, (1, 0))
        self.push(8, (1, 1), 1, (-1, 0))

    def end_own(self):
        self.arrived(5, (2, 0), 0, (-1, 0))
        self.arrived(6, (2, 0), 1, (1, 0))

    def end_pair(self):
        self.arrived(7, (2, 1), 0, (-1, 0))
        self.arrived(8, (2, 1), 1, (1, 0))

    def drain(self):
        for label, block, half, to in self.sent:
            self._copy(label, self.slot(*self._at(*block), half), *to).wait_send()


def bc_row(x, k):
    return jnp.broadcast_to(x[k : k + 1, :], (8, NB))


def bc_col(x, j):
    return jnp.broadcast_to(x[:, j : j + 1], (8, NB))


def inverse_factor(block):
    groups = NB // 8
    lane = lax.broadcasted_iota(jnp.int32, (8, NB), 1)
    sub = lax.broadcasted_iota(jnp.int32, (8, NB), 0)
    s = [block[8 * g : 8 * g + 8, :] for g in range(groups)]
    y = [jnp.where(lane == sub + 8 * g, 1.0, 0.0) for g in range(groups)]
    out = []
    for g0 in range(groups):
        top, inv = s[g0], y[g0]
        pivots = [bc_col(top, 8 * g0 + k) for k in range(8)]
        below = {g: [bc_col(s[g], 8 * g0 + k) for k in range(8)] for g in range(g0 + 1, groups)}
        scale = jnp.zeros((8, NB), jnp.float32)
        done = jnp.zeros((8, NB), jnp.float32)
        for k in range(8):
            pivot = bc_row(pivots[k], k)
            reciprocal = 1.0 / pivot
            here = sub == k
            f = jnp.where(here, 0.0, pivots[k] * reciprocal)
            scale = jnp.where(here, reciprocal, scale)
            done = jnp.where(here, inv * lax.rsqrt(pivot), done)
            for m in range(k + 1, 8):
                pivots[m] = pivots[m] - f * bc_row(pivots[m], k)
            top = top - f * bc_row(top, k)
            inv = inv - f * bc_row(inv, k)
        out.append(done)
        if g0 + 1 < groups:
            top, inv = top * scale, inv * scale
            tops = [bc_row(top, k) for k in range(8)]
            invs = [bc_row(inv, k) for k in range(8)]
            for g in range(g0 + 1, groups):
                t = [below[g][k] * tops[k] for k in range(8)]
                v = [below[g][k] * invs[k] for k in range(8)]
                while len(t) > 1:
                    t = [t[i] + t[i + 1] for i in range(0, len(t), 2)]
                    v = [v[i] + v[i + 1] for i in range(0, len(v), 2)]
                s[g] = s[g] - t[0]
                y[g] = y[g] - v[0]
    return jnp.concatenate(out, axis=0)


def whole_kernel(
    m_ref, mt_ref, out_ref,
    left, right, b1t, stage, a_ref, sq_ref, sh_ref, sl_ref, linv_ref, xh_ref, xl_ref,
    send, recv, swap_send, swap_recv, one_send, one_recv, local,
):
    row, col = lax.axis_index("row"), lax.axis_index("col")
    x, yh = lax.div(row, 2), lax.rem(row, 2)
    core, q = lax.rem(col, 2), lax.div(col, 2)
    yl, z = lax.div(q, 4), lax.rem(q, 4)
    depth, width = m_ref.shape
    height = 2 * width
    piece = SPAN // 2
    other = (row, q * 2 + 1 - core)

    def over_row(u, v):
        return (2 * u + v, col)

    def over_col(u, v):
        return (row, (4 * v + u) * 2 + core)

    def part(start, size, half):
        if half is None:
            return pl.ds(pl.multiple_of(start, 128), size)
        return pl.ds(pl.multiple_of(start + half * (size // 2), 128), size // 2)

    def right_slot(u, v, half):
        return right.at[2 * u + v, part(0, depth, half), :]

    def flip(a, b):
        return a + b - 2 * a * b

    r2, r1 = lax.div(x, 2), lax.rem(x, 2)

    def crossed(u, v):
        return 4 * flip(r2, v) + 2 * flip(r1, lax.div(u, 2)) + flip(yh, lax.rem(u, 2))

    cross = crossed(z, yl)
    blocks = {(du, dv): crossed(lax.rem(z + du + 4, 4), yl if dv == 0 else 1 - yl)
              for du in (-1, 0, 1, 2) for dv in (0, 1)}

    def left_slot(u, v, half, side=core):
        return left.at[crossed(u, v), part(side * width, width, half), :]

    def b1_slot(u, v, half, side=core):
        return b1t.at[2 * u + v, part(side * piece, piece, half), :]

    r_stream = Stream(0, send, recv, right_slot, over_row, x, yh)
    b_stream = Stream(1, send, recv, b1_slot, over_row, x, yh)
    l_stream = Stream(2, send, recv, left_slot, over_col, z, yl)
    order = ((0, 0), (0, 1), (-1, 0), (1, 0), (-1, 1), (1, 1), (2, 0), (2, 1))
    swaps = []

    def swap_copy(base, number, ref):
        place = base + number + l_stream.zero
        return pltpu.make_async_remote_copy(
            src_ref=ref, dst_ref=ref,
            send_sem=swap_send.at[place], recv_sem=swap_recv.at[place],
            device_id=other, device_id_type=MESH,
        )

    def swap_out(base, number):
        stream, slot = (b_stream, b1_slot) if base == 8 else (l_stream, left_slot)
        return swap_copy(base, number, slot(*stream._at(*order[number]), None))

    def swap(base, number):
        swap_out(base, number).start()
        swaps.append((base, number))

    def swapped(base, number):
        stream, slot = (b_stream, b1_slot) if base == 8 else (l_stream, left_slot)
        theirs = slot(*stream._at(*order[number]), None, 1 - core)
        swap_copy(base, number, theirs).wait_recv()

    def single(number, ref, target, place=None):
        return pltpu.make_async_remote_copy(
            src_ref=ref, dst_ref=ref if place is None else place,
            send_sem=one_send.at[number], recv_sem=one_recv.at[number],
            device_id=target, device_id_type=MESH,
        )

    own_right = pltpu.make_async_copy(m_ref, right.at[row], local.at[0])
    own_right.start()

    barrier = pltpu.get_barrier_semaphore()
    inside, across = (row, 2 * cross + core), (cross, col)
    friends = [
        over_row(lax.rem(x + 1, 4), yh), over_row(lax.rem(x + 3, 4), yh), over_row(x, 1 - yh),
        over_col(lax.rem(z + 1, 4), yl), over_col(lax.rem(z + 3, 4), yl), over_col(z, 1 - yl),
        other,
    ]
    for friend in friends:
        pl.semaphore_signal(barrier, inc=1, device_id=friend, device_id_type=MESH)

    moves_in, moves_across = row != 0, q != 0
    for moves, friend in ((moves_in, inside), (moves_across, across)):
        @pl.when(moves)
        def _(friend=friend):
            pl.semaphore_signal(barrier, inc=1, device_id=friend, device_id_type=MESH)

    for one in (0, 1):
        for two in (0, 1):
            here = jnp.logical_and(
                moves_in if one else row == 0, moves_across if two else q == 0
            )

            @pl.when(here)
            def _(count=len(friends) + one + two):
                pl.semaphore_wait(barrier, count)

    seed = jnp.logical_and(yl == 0, z == 0)
    spare = b1t.at[row, pl.ds(piece, width - piece), :]
    low = b1t.at[row, pl.ds(0, piece), :]
    high = b1t.at[row, pl.ds(width, SPAN - width), :]
    chunk = [b1_slot(x, yh, 0), b1_slot(x, yh, 1)]

    @pl.when(jnp.logical_and(seed, core == 0))
    def _():
        single(1, mt_ref.at[pl.ds(piece, width - piece), :], other, spare).start()
        copy = pltpu.make_async_copy(mt_ref.at[pl.ds(0, piece), :], low, local.at[2])
        copy.start()
        copy.wait()

    @pl.when(jnp.logical_and(seed, core == 1))
    def _():
        copy = pltpu.make_async_copy(mt_ref.at[pl.ds(0, SPAN - width), :], high, local.at[2])
        copy.start()
        copy.wait()
        single(1, spare, other).wait_recv()

    def down(h):
        single(4 + h, chunk[h], over_col(1, yl)).start()

    def up(h):
        single(6 + h, chunk[h], over_col(3, yl)).start()

    @pl.when(seed)
    def _():
        for h in range(2):
            single(2 + h, chunk[h], over_col(0, 1)).start()
            down(h)
            up(1 - h)

    def mine(h):
        return part(core * width, width, h)

    def along(h):
        at = part(0, width, h)
        return single(10 + h, mt_ref.at[at, :], inside, stage.at[at, :])

    def over(h, slot):
        return single(12 + h, stage.at[part(0, width, h), :], across, left.at[slot, mine(h), :])

    def still(h):
        return pltpu.make_async_copy(
            stage.at[part(0, width, h), :], left.at[cross, mine(h), :], local.at[3 + h]
        )

    @pl.when(moves_in)
    def _():
        along(0).start()
        along(1).start()

    @pl.when(row == 0)
    def _():
        pltpu.make_async_copy(mt_ref, stage, local.at[1]).start()

    own_right.wait()
    r_stream.push(1, (0, 0), None, (1, 0))
    r_stream.push(2, (0, 0), None, (-1, 0))

    @pl.when(jnp.logical_and(z == 0, yl == 1))
    def _():
        for h in range(2):
            single(2 + h, chunk[h], over_col(0, 0)).wait_recv()
            down(h)
            up(h)

    @pl.when(z == 1)
    def _():
        single(4, chunk[0], over_col(0, yl)).wait_recv()
        single(8, chunk[0], over_col(2, yl)).start()
        single(5, chunk[1], over_col(0, yl)).wait_recv()

    @pl.when(z == 3)
    def _():
        single(7, chunk[1], over_col(0, yl)).wait_recv()
        single(9, chunk[1], over_col(2, yl)).start()
        single(6, chunk[0], over_col(0, yl)).wait_recv()

    @pl.when(z == 2)
    def _():
        single(8, chunk[0], over_col(1, yl)).wait_recv()
        single(9, chunk[1], over_col(3, yl)).wait_recv()

    b_stream.send_own()
    swap(8, 0)

    @pl.when(row == 0)
    def _():
        pltpu.make_async_copy(mt_ref, stage, local.at[1]).wait()

    for h in range(2):
        @pl.when(moves_in)
        def _(h=h):
            along(h).wait_recv()

        @pl.when(moves_across)
        def _(h=h):
            over(h, row).start()

        @pl.when(q == 0)
        def _(h=h):
            still(h).start()

    r_stream.push(0, (0, 0), None, (0, 1))

    rows = 512

    def at_tile(tile):
        return pl.ds(pl.multiple_of(tile * rows, rows), rows)

    def gram(number):
        swapped(8, number)
        uu, vv = b_stream._at(*order[number])
        k = 2 * uu + vv

        def over_span(tile, carry):
            value = nt(b1t[k, at_tile(tile), :], b1t[k])
            if number == 0:
                a_ref[at_tile(tile), :] = value
            else:
                a_ref[at_tile(tile), :] += value
            return carry

        lax.fori_loop(0, SPAN // rows, over_span, 0)

    b_stream.send_pair()
    swap(8, 1)
    b_stream.relay_own()
    swap(8, 2)
    swap(8, 3)

    for h in range(2):
        @pl.when(moves_across)
        def _(h=h):
            over(h, cross).wait_recv()

        @pl.when(q == 0)
        def _(h=h):
            still(h).wait()

    l_stream.send_own()
    swap(0, 0)
    gram(0)
    gram(1)
    b_stream.relay_pair()
    swap(8, 4)
    swap(8, 5)
    r_stream.send_pair()
    r_stream.relay_own()
    gram(2)
    gram(3)
    l_stream.send_pair()
    swap(0, 1)
    l_stream.relay_own()
    swap(0, 2)
    swap(0, 3)
    b_stream.end_own()
    swap(8, 6)
    gram(4)
    gram(5)
    b_stream.end_pair()
    swap(8, 7)
    gram(6)
    gram(7)

    eye = jnp.where(
        lax.broadcasted_iota(jnp.int32, (NB, NB), 0) == lax.broadcasted_iota(jnp.int32, (NB, NB), 1),
        1.0, 0.0,
    )
    for b in range(BLOCKS):
        at = slice(b * NB, (b + 1) * NB)
        a_ref[at, at] += eye
    linv_ref[...] = jnp.zeros_like(linv_ref)
    tall = 256

    right_order = [2 * r_stream._at(*o)[0] + r_stream._at(*o)[1] for o in order]
    left_order = [blocks[o] for o in order]

    def choose(b, values):
        value = values[0]
        for i in range(1, BLOCKS):
            value = lax.select(b == i, values[i], value)
        return value

    sq_ref[...] = jnp.zeros_like(sq_ref)
    out_ref[...] = jnp.zeros_like(out_ref)
    half_rows = part(core * width, width, None)

    def factor_step(b, carry):
        r_stream.zero = l_stream.zero = b * 0

        @pl.when(b == 2)
        def _():
            l_stream.relay_pair()
            swap(0, 4)
            swap(0, 5)

        @pl.when(b == 3)
        def _():
            r_stream.relay_pair()

        @pl.when(b == 6)
        def _():
            r_stream.end_own()
            l_stream.end_own()
            swap(0, 6)

        @pl.when(b == 7)
        def _():
            r_stream.end_pair()
            l_stream.end_pair()
            swap(0, 7)

        at = pl.ds(pl.multiple_of(b * NB, NB), NB)
        y = inverse_factor(a_ref[at, at])
        linv_ref[at, at] = y
        kr, kl = choose(b, right_order), choose(b, left_order)
        sq_ref[...] += nn(b1t[kr], right[kr])
        lhs = left[kl, half_rows, :]
        out_ref[0:width, :] += nt(lhs, b1t[kl, 0:width, :])
        out_ref[width:height, 0 : SPAN - width] += nt(lhs, b1t[kl, width:SPAN, :])
        below = lax.broadcasted_iota(jnp.int32, (SPAN, NB), 0) >= (b + 1) * NB
        panel = three(nt, split(a_ref[:, at]), split(y))
        panel = jnp.where(below, panel, 0.0)
        a_ref[:, at] = panel
        xh_ref[:, 0:NB], xl_ref[:, 0:NB] = split(panel)

        def update(tile, c):
            part_rows = pl.ds(pl.multiple_of(tile * tall, tall), tall)
            a_ref[part_rows, :] -= three(
                nt,
                (xh_ref[part_rows, 0:NB], xl_ref[part_rows, 0:NB]),
                (xh_ref[:, 0:NB], xl_ref[:, 0:NB]),
            )
            return c

        lax.fori_loop((b + 1) // 2, SPAN // tall, update, 0)

        return carry

    lax.fori_loop(0, BLOCKS, factor_step, 0)
    r_stream.zero = l_stream.zero = 0

    first = row * height + core * width
    for t in range(width // tall):
        to = pl.ds(pl.multiple_of(core * width + t * tall, tall), tall)
        for base, lo, hi in ((0, 0, width), (width, width, SPAN)):
            shape = (tall, hi - lo)
            srow = first + t * tall + lax.broadcasted_iota(jnp.int32, shape, 0)
            scol = lo + lax.broadcasted_iota(jnp.int32, shape, 1)
            strip = out_ref[base + t * tall : base + (t + 1) * tall, 0 : hi - lo]
            strip += jnp.where(srow == scol, 1.0, 0.0)
            sh_ref[to, lo:hi], sl_ref[to, lo:hi] = split(strip)

    size = NB
    while size < SPAN:
        for lo in range(0, SPAN, 2 * size):
            one, two = slice(lo, lo + size), slice(lo + size, lo + 2 * size)
            inner = three(nn, split(a_ref[two, one]), split(linv_ref[one, one]))
            linv_ref[two, one] = -three(nn, split(linv_ref[two, two]), split(inner))
        size *= 2

    def strips(side):
        at = part(side * width, width, None)
        return [single(14 + i, ref.at[at, :], other) for i, ref in enumerate((sh_ref, sl_ref))]

    for copy in strips(core):
        copy.start()

    cols = col * width + lax.broadcasted_iota(jnp.int32, (tall, width), 1)
    for b in range(SPAN // tall):
        at = slice(b * tall, (b + 1) * tall)
        upto = slice(0, (b + 1) * tall)
        solved = three(nn, split(linv_ref[at, upto]), split(sq_ref[upto, :]))
        unit = jnp.where(b * tall + lax.broadcasted_iota(jnp.int32, (tall, width), 0) == cols, 1.0, 0.0)
        xh_ref[at, :], xl_ref[at, :] = split(jnp.where(cols < SPAN, unit, solved))
    for b in range(SPAN // tall):
        at = slice(b * tall, (b + 1) * tall)
        onward = slice(b * tall, SPAN)
        sq_ref[at, :] = three(tn, split(linv_ref[onward, at]), (xh_ref[onward, :], xl_ref[onward, :]))
    for b in range(SPAN // tall):
        at = slice(b * tall, (b + 1) * tall)
        xh_ref[at, :], xl_ref[at, :] = split(sq_ref[at, :])

    for number in range(8):
        swapped(0, number)

    def over_rows(t, carry):
        at = pl.ds(pl.multiple_of(t * tall, tall), tall)
        value = nn(left[0, at, :], right[0])
        for i in range(1, 8):
            value += nn(left[i, at, :], right[i])
        out_ref[at, :] = value
        return carry

    lax.fori_loop(0, height // tall, over_rows, 0)
    for copy in strips(1 - core):
        copy.wait_recv()

    def finish(t, carry):
        at = pl.ds(pl.multiple_of(t * tall, tall), tall)
        first = row * height + t * tall
        grow = first + lax.broadcasted_iota(jnp.int32, (tall, width), 0)
        gcol = col * width + lax.broadcasted_iota(jnp.int32, (tall, width), 1)
        value = three(nn, (sh_ref[at, :], sl_ref[at, :]), (xh_ref[...], xl_ref[...]))
        system = out_ref[at, :] + jnp.where(grow == gcol, 1.0, 0.0)
        lead = jnp.where(grow >= gcol, value, 0.0)
        rest = jnp.where(grow < SPAN, 0.0, system - value)
        out_ref[at, :] = jnp.where(gcol < SPAN, lead, rest)
        return carry

    lax.fori_loop(0, height // tall, finish, 0)

    for stream in (r_stream, b_stream, l_stream):
        stream.drain()
    for base, number in swaps:
        swap_out(base, number).wait_send()

    for copy in strips(core):
        copy.wait_send()

    for h in range(2):
        @pl.when(moves_in)
        def _(h=h):
            along(h).wait_send()

        @pl.when(moves_across)
        def _(h=h):
            over(h, row).wait_send()

    @pl.when(jnp.logical_and(seed, core == 0))
    def _():
        single(1, mt_ref.at[pl.ds(piece, width - piece), :], other, spare).wait_send()

    @pl.when(seed)
    def _():
        for h in range(2):
            single(2 + h, chunk[h], over_col(0, 1)).wait_send()

    @pl.when(z == 0)
    def _():
        for h in range(2):
            single(4 + h, chunk[h], over_col(1, yl)).wait_send()
            single(6 + h, chunk[h], over_col(3, yl)).wait_send()

    @pl.when(z == 1)
    def _():
        single(8, chunk[0], over_col(2, yl)).wait_send()

    @pl.when(z == 3)
    def _():
        single(9, chunk[1], over_col(2, yl)).wait_send()


def whole(masked, transposed):
    depth, width = masked.shape
    height = 2 * width
    f32, bf16 = jnp.float32, jnp.bfloat16
    dma = pltpu.SemaphoreType.DMA
    hbm, vmem = pl.BlockSpec(memory_space=pl.ANY), pl.BlockSpec(memory_space=pltpu.VMEM)
    return pl.pallas_call(
        whole_kernel,
        out_shape=jax.ShapeDtypeStruct((height, width), f32),
        in_specs=[hbm, hbm],
        out_specs=vmem,
        scratch_shapes=[
            pltpu.VMEM((8, height, depth), bf16),
            pltpu.VMEM((8, depth, width), bf16),
            pltpu.VMEM((8, SPAN, depth), bf16),
            pltpu.VMEM((width, depth), bf16),
            pltpu.VMEM((SPAN, SPAN), f32),
            pltpu.VMEM((SPAN, width), f32),
            pltpu.VMEM((height, SPAN), bf16),
            pltpu.VMEM((height, SPAN), bf16),
            pltpu.VMEM((SPAN, SPAN), f32),
            pltpu.VMEM((SPAN, width), bf16),
            pltpu.VMEM((SPAN, width), bf16),
            dma((3, 9)), dma((3, 9)),
            dma((16,)), dma((16,)),
            dma((16,)), dma((16,)),
            dma((5,)),
        ],
        compiler_params=pltpu.CompilerParams(
            collective_id=0, has_side_effects=True, vmem_limit_bytes=VMEM_LIMIT
        ),
        name="whole",
    )(masked, transposed)


def expand_tiles(blocks):
    return jnp.repeat(jnp.repeat(blocks, TILE, axis=0), TILE, axis=1)


def on_device(b_values, tile_mask):
    row_index = lax.axis_index("row")
    col_index = lax.axis_index("col")
    depth, width = b_values.shape
    occupancy = lax.dynamic_slice(
        tile_mask,
        (row_index * (depth // TILE), col_index * (width // TILE)),
        (depth // TILE, width // TILE),
    )
    masked = b_values * expand_tiles(occupancy).astype(jnp.bfloat16)
    return whole(masked, masked.T)


def solution(mesh):
    return jax.shard_map(
        on_device,
        mesh=mesh,
        in_specs=(P("row", "col"), P()),
        out_specs=P("row", "col"),
        check_vma=False,
    )
```

```python
import functools

import jax
import jax.numpy as jnp
from jax import lax
from jax.experimental import pallas as pl
from jax.experimental.pallas import tpu as pltpu
from jax.sharding import PartitionSpec as P

TILE = 256
PANEL = 512
SPAN = 2 * PANEL
NB = 128
BLOCKS = SPAN // NB
MESH = pl.DeviceIdType.MESH
VMEM_LIMIT = 66_000_000


def nn(a, b):
    return lax.dot_general(a, b, (((1,), (0,)), ((), ())), preferred_element_type=jnp.float32)


def nt(a, b):
    return lax.dot_general(a, b, (((1,), (1,)), ((), ())), preferred_element_type=jnp.float32)


def tn(a, b):
    return lax.dot_general(a, b, (((0,), (0,)), ((), ())), preferred_element_type=jnp.float32)


def split(value):
    high = value.astype(jnp.bfloat16)
    return high, (value - high.astype(jnp.float32)).astype(jnp.bfloat16)


def three(dot, a, b):
    (ah, al), (bh, bl) = a, b
    return dot(ah, bh) + (dot(al, bh) + dot(ah, bl))


class Stream:
    def __init__(self, index, send, recv, slot, device, u, v):
        self.index, self.send, self.recv = index, send, recv
        self.slot, self.device, self.u, self.v = slot, device, u, v
        self.sent = []
        self.ring = {du: lax.rem(u + du + 4, 4) for du in (-1, 0, 1, 2)}
        self.pair = {0: v, 1: 1 - v}
        self.zero = 0

    def _at(self, du, dv):
        return self.ring[du], self.pair[dv]

    def _copy(self, label, ref, du, dv):
        uu, vv = self._at(du, dv)
        return pltpu.make_async_remote_copy(
            src_ref=ref,
            dst_ref=ref,
            send_sem=self.send.at[self.index + self.zero, label + self.zero],
            recv_sem=self.recv.at[self.index + self.zero, label + self.zero],
            device_id=self.device(uu, vv),
            device_id_type=MESH,
        )

    def push(self, label, block, half, to):
        copy = self._copy(label, self.slot(*self._at(*block), half), *to)
        copy.start()
        self.sent.append((label, block, half, to))

    def arrived(self, label, block, half, source):
        self._copy(label, self.slot(*self._at(*block), half), *source).wait_recv()

    def send_own(self):
        self.push(0, (0, 0), None, (0, 1))
        self.push(1, (0, 0), None, (1, 0))
        self.push(2, (0, 0), None, (-1, 0))

    def send_pair(self):
        self.arrived(0, (0, 1), None, (0, 1))
        self.push(3, (0, 1), None, (1, 0))
        self.push(4, (0, 1), None, (-1, 0))

    def relay_own(self):
        self.arrived(1, (-1, 0), None, (-1, 0))
        self.push(5, (-1, 0), 0, (1, 0))
        self.arrived(2, (1, 0), None, (1, 0))
        self.push(6, (1, 0), 1, (-1, 0))

    def relay_pair(self):
        self.arrived(3, (-1, 1), None, (-1, 0))
        self.push(7, (-1, 1), 0, (1, 0))
        self.arrived(4, (1, 1), None, (1, 0))
        self.push(8, (1, 1), 1, (-1, 0))

    def end_own(self):
        self.arrived(5, (2, 0), 0, (-1, 0))
        self.arrived(6, (2, 0), 1, (1, 0))

    def end_pair(self):
        self.arrived(7, (2, 1), 0, (-1, 0))
        self.arrived(8, (2, 1), 1, (1, 0))

    def drain(self):
        for label, block, half, to in self.sent:
            self._copy(label, self.slot(*self._at(*block), half), *to).wait_send()


def bc_row(x, k):
    return jnp.broadcast_to(x[k : k + 1, :], (8, NB))


def bc_col(x, j):
    return jnp.broadcast_to(x[:, j : j + 1], (8, NB))


def inverse_factor(block):
    groups = NB // 8
    lane = lax.broadcasted_iota(jnp.int32, (8, NB), 1)
    sub = lax.broadcasted_iota(jnp.int32, (8, NB), 0)
    s = [block[8 * g : 8 * g + 8, :] for g in range(groups)]
    y = [jnp.where(lane == sub + 8 * g, 1.0, 0.0) for g in range(groups)]
    out = []
    for g0 in range(groups):
        top, inv = s[g0], y[g0]
        pivots = [bc_col(top, 8 * g0 + k) for k in range(8)]
        below = {g: [bc_col(s[g], 8 * g0 + k) for k in range(8)] for g in range(g0 + 1, groups)}
        scale = jnp.zeros((8, NB), jnp.float32)
        done = jnp.zeros((8, NB), jnp.float32)
        for k in range(8):
            pivot = bc_row(pivots[k], k)
            reciprocal = 1.0 / pivot
            here = sub == k
            f = jnp.where(here, 0.0, pivots[k] * reciprocal)
            scale = jnp.where(here, reciprocal, scale)
            done = jnp.where(here, inv * lax.rsqrt(pivot), done)
            for m in range(k + 1, 8):
                pivots[m] = pivots[m] - f * bc_row(pivots[m], k)
            top = top - f * bc_row(top, k)
            inv = inv - f * bc_row(inv, k)
        out.append(done)
        if g0 + 1 < groups:
            top, inv = top * scale, inv * scale
            tops = [bc_row(top, k) for k in range(8)]
            invs = [bc_row(inv, k) for k in range(8)]
            for g in range(g0 + 1, groups):
                t = [below[g][k] * tops[k] for k in range(8)]
                v = [below[g][k] * invs[k] for k in range(8)]
                while len(t) > 1:
                    t = [t[i] + t[i + 1] for i in range(0, len(t), 2)]
                    v = [v[i] + v[i + 1] for i in range(0, len(v), 2)]
                s[g] = s[g] - t[0]
                y[g] = y[g] - v[0]
    return jnp.concatenate(out, axis=0)


def whole_kernel(
    m_ref, mt_ref, out_ref,
    left, right, b1t, stage, a_ref, sq_ref, sh_ref, sl_ref, linv_ref, xh_ref, xl_ref,
    send, recv, swap_send, swap_recv, one_send, one_recv, local,
):
    row, col = lax.axis_index("row"), lax.axis_index("col")
    x, yh = lax.div(row, 2), lax.rem(row, 2)
    core, q = lax.rem(col, 2), lax.div(col, 2)
    yl, z = lax.div(q, 4), lax.rem(q, 4)
    depth, width = m_ref.shape
    height = 2 * width
    piece = SPAN // 2
    other = (row, q * 2 + 1 - core)

    def over_row(u, v):
        return (2 * u + v, col)

    def over_col(u, v):
        return (row, (4 * v + u) * 2 + core)

    def part(start, size, half):
        if half is None:
            return pl.ds(pl.multiple_of(start, 128), size)
        return pl.ds(pl.multiple_of(start + half * (size // 2), 128), size // 2)

    def right_slot(u, v, half):
        return right.at[2 * u + v, part(0, depth, half), :]

    def flip(a, b):
        return a + b - 2 * a * b

    r2, r1 = lax.div(x, 2), lax.rem(x, 2)

    def crossed(u, v):
        return 4 * flip(r2, v) + 2 * flip(r1, lax.div(u, 2)) + flip(yh, lax.rem(u, 2))

    cross = crossed(z, yl)
    blocks = {(du, dv): crossed(lax.rem(z + du + 4, 4), yl if dv == 0 else 1 - yl)
              for du in (-1, 0, 1, 2) for dv in (0, 1)}

    def left_slot(u, v, half, side=core):
        return left.at[crossed(u, v), part(side * width, width, half), :]

    def b1_slot(u, v, half, side=core):
        return b1t.at[2 * u + v, part(side * piece, piece, half), :]

    r_stream = Stream(0, send, recv, right_slot, over_row, x, yh)
    b_stream = Stream(1, send, recv, b1_slot, over_row, x, yh)
    l_stream = Stream(2, send, recv, left_slot, over_col, z, yl)
    order = ((0, 0), (0, 1), (-1, 0), (1, 0), (-1, 1), (1, 1), (2, 0), (2, 1))
    swaps = []

    def swap_copy(base, number, ref):
        place = base + number + l_stream.zero
        return pltpu.make_async_remote_copy(
            src_ref=ref, dst_ref=ref,
            send_sem=swap_send.at[place], recv_sem=swap_recv.at[place],
            device_id=other, device_id_type=MESH,
        )

    def swap_out(base, number):
        stream, slot = (b_stream, b1_slot) if base == 8 else (l_stream, left_slot)
        return swap_copy(base, number, slot(*stream._at(*order[number]), None))

    def swap(base, number):
        swap_out(base, number).start()
        swaps.append((base, number))

    def swapped(base, number):
        stream, slot = (b_stream, b1_slot) if base == 8 else (l_stream, left_slot)
        theirs = slot(*stream._at(*order[number]), None, 1 - core)
        swap_copy(base, number, theirs).wait_recv()

    def single(number, ref, target, place=None):
        return pltpu.make_async_remote_copy(
            src_ref=ref, dst_ref=ref if place is None else place,
            send_sem=one_send.at[number], recv_sem=one_recv.at[number],
            device_id=target, device_id_type=MESH,
        )

    own_right = pltpu.make_async_copy(m_ref, right.at[row], local.at[0])
    own_right.start()

    barrier = pltpu.get_barrier_semaphore()
    inside, across = (row, 2 * cross + core), (cross, col)
    friends = [
        over_row(lax.rem(x + 1, 4), yh), over_row(lax.rem(x + 3, 4), yh), over_row(x, 1 - yh),
        over_col(lax.rem(z + 1, 4), yl), over_col(lax.rem(z + 3, 4), yl), over_col(z, 1 - yl),
        other,
    ]
    for friend in friends:
        pl.semaphore_signal(barrier, inc=1, device_id=friend, device_id_type=MESH)

    moves_in, moves_across = row != 0, q != 0
    for moves, friend in ((moves_in, inside), (moves_across, across)):
        @pl.when(moves)
        def _(friend=friend):
            pl.semaphore_signal(barrier, inc=1, device_id=friend, device_id_type=MESH)

    for one in (0, 1):
        for two in (0, 1):
            here = jnp.logical_and(
                moves_in if one else row == 0, moves_across if two else q == 0
            )

            @pl.when(here)
            def _(count=len(friends) + one + two):
                pl.semaphore_wait(barrier, count)

    seed = jnp.logical_and(yl == 0, z == 0)
    spare = b1t.at[row, pl.ds(piece, width - piece), :]
    low = b1t.at[row, pl.ds(0, piece), :]
    high = b1t.at[row, pl.ds(width, SPAN - width), :]
    chunk = [b1_slot(x, yh, 0), b1_slot(x, yh, 1)]

    @pl.when(jnp.logical_and(seed, core == 0))
    def _():
        single(1, mt_ref.at[pl.ds(piece, width - piece), :], other, spare).start()
        copy = pltpu.make_async_copy(mt_ref.at[pl.ds(0, piece), :], low, local.at[2])
        copy.start()
        copy.wait()

    @pl.when(jnp.logical_and(seed, core == 1))
    def _():
        copy = pltpu.make_async_copy(mt_ref.at[pl.ds(0, SPAN - width), :], high, local.at[2])
        copy.start()
        copy.wait()
        single(1, spare, other).wait_recv()

    def down(h):
        single(4 + h, chunk[h], over_col(1, yl)).start()

    def up(h):
        single(6 + h, chunk[h], over_col(3, yl)).start()

    @pl.when(seed)
    def _():
        for h in range(2):
            single(2 + h, chunk[h], over_col(0, 1)).start()
            down(h)
            up(1 - h)

    def mine(h):
        return part(core * width, width, h)

    def along(h):
        at = part(0, width, h)
        return single(10 + h, mt_ref.at[at, :], inside, stage.at[at, :])

    def over(h, slot):
        return single(12 + h, stage.at[part(0, width, h), :], across, left.at[slot, mine(h), :])

    def still(h):
        return pltpu.make_async_copy(
            stage.at[part(0, width, h), :], left.at[cross, mine(h), :], local.at[3 + h]
        )

    @pl.when(moves_in)
    def _():
        along(0).start()
        along(1).start()

    @pl.when(row == 0)
    def _():
        pltpu.make_async_copy(mt_ref, stage, local.at[1]).start()

    own_right.wait()
    r_stream.push(0, (0, 0), None, (0, 1))
    r_stream.push(1, (0, 0), None, (1, 0))
    r_stream.push(2, (0, 0), None, (-1, 0))

    @pl.when(jnp.logical_and(z == 0, yl == 1))
    def _():
        for h in range(2):
            single(2 + h, chunk[h], over_col(0, 0)).wait_recv()
            down(h)
            up(h)

    @pl.when(z == 1)
    def _():
        single(4, chunk[0], over_col(0, yl)).wait_recv()
        single(8, chunk[0], over_col(2, yl)).start()
        single(5, chunk[1], over_col(0, yl)).wait_recv()

    @pl.when(z == 3)
    def _():
        single(7, chunk[1], over_col(0, yl)).wait_recv()
        single(9, chunk[1], over_col(2, yl)).start()
        single(6, chunk[0], over_col(0, yl)).wait_recv()

    @pl.when(row == 0)
    def _():
        pltpu.make_async_copy(mt_ref, stage, local.at[1]).wait()

    for h in range(2):
        @pl.when(moves_in)
        def _(h=h):
            along(h).wait_recv()

        @pl.when(moves_across)
        def _(h=h):
            over(h, row).start()

        @pl.when(q == 0)
        def _(h=h):
            still(h).start()

    @pl.when(z == 2)
    def _():
        single(8, chunk[0], over_col(1, yl)).wait_recv()
        single(9, chunk[1], over_col(3, yl)).wait_recv()

    b_stream.send_own()
    swap(8, 0)

    rows = 512

    def at_tile(tile):
        return pl.ds(pl.multiple_of(tile * rows, rows), rows)

    def gram(number):
        swapped(8, number)
        uu, vv = b_stream._at(*order[number])
        k = 2 * uu + vv

        def over_span(tile, carry):
            value = nt(b1t[k, at_tile(tile), :], b1t[k])
            if number == 0:
                a_ref[at_tile(tile), :] = value
            else:
                a_ref[at_tile(tile), :] += value
            return carry

        lax.fori_loop(0, SPAN // rows, over_span, 0)

    b_stream.send_pair()
    swap(8, 1)
    for h in range(2):
        @pl.when(moves_across)
        def _(h=h):
            over(h, cross).wait_recv()

        @pl.when(q == 0)
        def _(h=h):
            still(h).wait()

    l_stream.send_own()
    swap(0, 0)
    b_stream.relay_own()
    swap(8, 2)
    swap(8, 3)
    gram(0)
    gram(1)
    b_stream.relay_pair()
    swap(8, 4)
    swap(8, 5)
    r_stream.relay_own()
    r_stream.send_pair()
    gram(2)
    gram(3)
    l_stream.send_pair()
    swap(0, 1)
    l_stream.relay_own()
    swap(0, 2)
    swap(0, 3)
    b_stream.end_own()
    swap(8, 6)
    gram(4)
    gram(5)
    b_stream.end_pair()
    swap(8, 7)
    gram(6)
    gram(7)

    eye = jnp.where(
        lax.broadcasted_iota(jnp.int32, (NB, NB), 0) == lax.broadcasted_iota(jnp.int32, (NB, NB), 1),
        1.0, 0.0,
    )
    for b in range(BLOCKS):
        at = slice(b * NB, (b + 1) * NB)
        a_ref[at, at] += eye
    linv_ref[...] = jnp.zeros_like(linv_ref)
    tall = 256

    right_order = [2 * r_stream._at(*o)[0] + r_stream._at(*o)[1] for o in order]
    left_order = [blocks[o] for o in order]

    def choose(b, values):
        value = values[0]
        for i in range(1, BLOCKS):
            value = lax.select(b == i, values[i], value)
        return value

    sq_ref[...] = jnp.zeros_like(sq_ref)
    out_ref[...] = jnp.zeros_like(out_ref)
    half_rows = part(core * width, width, None)

    def factor_step(b, carry):
        r_stream.zero = l_stream.zero = b * 0

        @pl.when(b == 2)
        def _():
            l_stream.relay_pair()
            swap(0, 4)
            swap(0, 5)

        @pl.when(b == 3)
        def _():
            r_stream.relay_pair()

        @pl.when(b == 6)
        def _():
            r_stream.end_own()
            l_stream.end_own()
            swap(0, 6)

        @pl.when(b == 7)
        def _():
            r_stream.end_pair()
            l_stream.end_pair()
            swap(0, 7)

        at = pl.ds(pl.multiple_of(b * NB, NB), NB)
        y = inverse_factor(a_ref[at, at])
        linv_ref[at, at] = y
        kr, kl = choose(b, right_order), choose(b, left_order)
        sq_ref[...] += nn(b1t[kr], right[kr])
        lhs = left[kl, half_rows, :]
        out_ref[0:width, :] += nt(lhs, b1t[kl, 0:width, :])
        out_ref[width:height, 0 : SPAN - width] += nt(lhs, b1t[kl, width:SPAN, :])
        below = lax.broadcasted_iota(jnp.int32, (SPAN, NB), 0) >= (b + 1) * NB
        panel = three(nt, split(a_ref[:, at]), split(y))
        panel = jnp.where(below, panel, 0.0)
        a_ref[:, at] = panel
        xh_ref[:, 0:NB], xl_ref[:, 0:NB] = split(panel)

        def update(tile, c):
            part_rows = pl.ds(pl.multiple_of(tile * tall, tall), tall)
            a_ref[part_rows, :] -= three(
                nt,
                (xh_ref[part_rows, 0:NB], xl_ref[part_rows, 0:NB]),
                (xh_ref[:, 0:NB], xl_ref[:, 0:NB]),
            )
            return c

        lax.fori_loop((b + 1) // 2, SPAN // tall, update, 0)

        return carry

    lax.fori_loop(0, BLOCKS, factor_step, 0)
    r_stream.zero = l_stream.zero = 0

    first = row * height + core * width
    for t in range(width // tall):
        to = pl.ds(pl.multiple_of(core * width + t * tall, tall), tall)
        for base, lo, hi in ((0, 0, width), (width, width, SPAN)):
            shape = (tall, hi - lo)
            srow = first + t * tall + lax.broadcasted_iota(jnp.int32, shape, 0)
            scol = lo + lax.broadcasted_iota(jnp.int32, shape, 1)
            strip = out_ref[base + t * tall : base + (t + 1) * tall, 0 : hi - lo]
            strip += jnp.where(srow == scol, 1.0, 0.0)
            sh_ref[to, lo:hi], sl_ref[to, lo:hi] = split(strip)

    size = NB
    while size < SPAN:
        for lo in range(0, SPAN, 2 * size):
            one, two = slice(lo, lo + size), slice(lo + size, lo + 2 * size)
            inner = three(nn, split(a_ref[two, one]), split(linv_ref[one, one]))
            linv_ref[two, one] = -three(nn, split(linv_ref[two, two]), split(inner))
        size *= 2

    def strips(side):
        at = part(side * width, width, None)
        return [single(14 + i, ref.at[at, :], other) for i, ref in enumerate((sh_ref, sl_ref))]

    for copy in strips(core):
        copy.start()

    cols = col * width + lax.broadcasted_iota(jnp.int32, (tall, width), 1)
    for b in range(SPAN // tall):
        at = slice(b * tall, (b + 1) * tall)
        upto = slice(0, (b + 1) * tall)
        solved = three(nn, split(linv_ref[at, upto]), split(sq_ref[upto, :]))
        unit = jnp.where(b * tall + lax.broadcasted_iota(jnp.int32, (tall, width), 0) == cols, 1.0, 0.0)
        xh_ref[at, :], xl_ref[at, :] = split(jnp.where(cols < SPAN, unit, solved))
    for b in range(SPAN // tall):
        at = slice(b * tall, (b + 1) * tall)
        onward = slice(b * tall, SPAN)
        sq_ref[at, :] = three(tn, split(linv_ref[onward, at]), (xh_ref[onward, :], xl_ref[onward, :]))
    for b in range(SPAN // tall):
        at = slice(b * tall, (b + 1) * tall)
        xh_ref[at, :], xl_ref[at, :] = split(sq_ref[at, :])

    for number in range(8):
        swapped(0, number)

    def over_rows(t, carry):
        at = pl.ds(pl.multiple_of(t * tall, tall), tall)
        value = nn(left[0, at, :], right[0])
        for i in range(1, 8):
            value += nn(left[i, at, :], right[i])
        out_ref[at, :] = value
        return carry

    lax.fori_loop(0, height // tall, over_rows, 0)
    for copy in strips(1 - core):
        copy.wait_recv()

    def finish(t, carry):
        at = pl.ds(pl.multiple_of(t * tall, tall), tall)
        first = row * height + t * tall
        grow = first + lax.broadcasted_iota(jnp.int32, (tall, width), 0)
        gcol = col * width + lax.broadcasted_iota(jnp.int32, (tall, width), 1)
        value = nn(sh_ref[at, :], xh_ref[...]) + nn(sh_ref[at, :], xl_ref[...])
        system = out_ref[at, :] + jnp.where(grow == gcol, 1.0, 0.0)
        lead = jnp.where(grow >= gcol, value, 0.0)
        rest = jnp.where(grow < SPAN, 0.0, system - value)
        out_ref[at, :] = jnp.where(gcol < SPAN, lead, rest)

        @pl.when(col < 2)
        def _():
            low = nn(sl_ref[at, :], xh_ref[...])
            keep = jnp.logical_and(gcol < SPAN, grow >= gcol)
            out_ref[at, :] += jnp.where(keep, low, 0.0)

        return carry

    lax.fori_loop(0, height // tall, finish, 0)

    for stream in (r_stream, b_stream, l_stream):
        stream.drain()
    for base, number in swaps:
        swap_out(base, number).wait_send()

    for copy in strips(core):
        copy.wait_send()

    for h in range(2):
        @pl.when(moves_in)
        def _(h=h):
            along(h).wait_send()

        @pl.when(moves_across)
        def _(h=h):
            over(h, row).wait_send()

    @pl.when(jnp.logical_and(seed, core == 0))
    def _():
        single(1, mt_ref.at[pl.ds(piece, width - piece), :], other, spare).wait_send()

    @pl.when(seed)
    def _():
        for h in range(2):
            single(2 + h, chunk[h], over_col(0, 1)).wait_send()

    @pl.when(z == 0)
    def _():
        for h in range(2):
            single(4 + h, chunk[h], over_col(1, yl)).wait_send()
            single(6 + h, chunk[h], over_col(3, yl)).wait_send()

    @pl.when(z == 1)
    def _():
        single(8, chunk[0], over_col(2, yl)).wait_send()

    @pl.when(z == 3)
    def _():
        single(9, chunk[1], over_col(2, yl)).wait_send()


def whole(masked, transposed):
    depth, width = masked.shape
    height = 2 * width
    f32, bf16 = jnp.float32, jnp.bfloat16
    dma = pltpu.SemaphoreType.DMA
    hbm, vmem = pl.BlockSpec(memory_space=pl.ANY), pl.BlockSpec(memory_space=pltpu.VMEM)
    return pl.pallas_call(
        whole_kernel,
        out_shape=jax.ShapeDtypeStruct((height, width), f32),
        in_specs=[hbm, hbm],
        out_specs=vmem,
        scratch_shapes=[
            pltpu.VMEM((8, height, depth), bf16),
            pltpu.VMEM((8, depth, width), bf16),
            pltpu.VMEM((8, SPAN, depth), bf16),
            pltpu.VMEM((width, depth), bf16),
            pltpu.VMEM((SPAN, SPAN), f32),
            pltpu.VMEM((SPAN, width), f32),
            pltpu.VMEM((height, SPAN), bf16),
            pltpu.VMEM((height, SPAN), bf16),
            pltpu.VMEM((SPAN, SPAN), f32),
            pltpu.VMEM((SPAN, width), bf16),
            pltpu.VMEM((SPAN, width), bf16),
            dma((3, 9)), dma((3, 9)),
            dma((16,)), dma((16,)),
            dma((16,)), dma((16,)),
            dma((5,)),
        ],
        compiler_params=pltpu.CompilerParams(
            collective_id=0, has_side_effects=True, vmem_limit_bytes=VMEM_LIMIT
        ),
        name="whole",
    )(masked, transposed)


def expand_tiles(blocks):
    return jnp.repeat(jnp.repeat(blocks, TILE, axis=0), TILE, axis=1)


def on_device(b_values, tile_mask):
    row_index = lax.axis_index("row")
    col_index = lax.axis_index("col")
    depth, width = b_values.shape
    occupancy = lax.dynamic_slice(
        tile_mask,
        (row_index * (depth // TILE), col_index * (width // TILE)),
        (depth // TILE, width // TILE),
    )
    masked = b_values * expand_tiles(occupancy).astype(jnp.bfloat16)
    return whole(masked, masked.T)


def solution(mesh):
    return jax.shard_map(
        on_device,
        mesh=mesh,
        in_specs=(P("row", "col"), P()),
        out_specs=P("row", "col"),
        check_vma=False,
    )
```

```python
import functools

import jax
import jax.numpy as jnp
from jax import lax
from jax.experimental import pallas as pl
from jax.experimental.pallas import tpu as pltpu
from jax.sharding import PartitionSpec as P

TILE = 256
PANEL = 512
SPAN = 2 * PANEL
NB = 128
BLOCKS = SPAN // NB
MESH = pl.DeviceIdType.MESH
VMEM_LIMIT = 66_000_000


def nn(a, b):
    return lax.dot_general(a, b, (((1,), (0,)), ((), ())), preferred_element_type=jnp.float32)


def nt(a, b):
    return lax.dot_general(a, b, (((1,), (1,)), ((), ())), preferred_element_type=jnp.float32)


def tn(a, b):
    return lax.dot_general(a, b, (((0,), (0,)), ((), ())), preferred_element_type=jnp.float32)


def split(value):
    high = value.astype(jnp.bfloat16)
    return high, (value - high.astype(jnp.float32)).astype(jnp.bfloat16)


def three(dot, a, b):
    (ah, al), (bh, bl) = a, b
    return dot(ah, bh) + (dot(al, bh) + dot(ah, bl))


class Stream:
    def __init__(self, index, send, recv, slot, device, u, v):
        self.index, self.send, self.recv = index, send, recv
        self.slot, self.device, self.u, self.v = slot, device, u, v
        self.sent = []
        self.ring = {du: lax.rem(u + du + 4, 4) for du in (-1, 0, 1, 2)}
        self.pair = {0: v, 1: 1 - v}
        self.zero = 0

    def _at(self, du, dv):
        return self.ring[du], self.pair[dv]

    def _copy(self, label, ref, du, dv):
        uu, vv = self._at(du, dv)
        return pltpu.make_async_remote_copy(
            src_ref=ref,
            dst_ref=ref,
            send_sem=self.send.at[self.index + self.zero, label + self.zero],
            recv_sem=self.recv.at[self.index + self.zero, label + self.zero],
            device_id=self.device(uu, vv),
            device_id_type=MESH,
        )

    def push(self, label, block, half, to):
        copy = self._copy(label, self.slot(*self._at(*block), half), *to)
        copy.start()
        self.sent.append((label, block, half, to))

    def arrived(self, label, block, half, source):
        self._copy(label, self.slot(*self._at(*block), half), *source).wait_recv()

    def send_own(self):
        self.push(0, (0, 0), None, (0, 1))
        self.push(1, (0, 0), None, (1, 0))
        self.push(2, (0, 0), None, (-1, 0))

    def send_pair(self):
        self.arrived(0, (0, 1), None, (0, 1))
        self.push(3, (0, 1), None, (1, 0))
        self.push(4, (0, 1), None, (-1, 0))

    def relay_own(self):
        self.arrived(1, (-1, 0), None, (-1, 0))
        self.push(5, (-1, 0), 0, (1, 0))
        self.arrived(2, (1, 0), None, (1, 0))
        self.push(6, (1, 0), 1, (-1, 0))

    def relay_pair(self):
        self.arrived(3, (-1, 1), None, (-1, 0))
        self.push(7, (-1, 1), 0, (1, 0))
        self.arrived(4, (1, 1), None, (1, 0))
        self.push(8, (1, 1), 1, (-1, 0))

    def end_own(self):
        self.arrived(5, (2, 0), 0, (-1, 0))
        self.arrived(6, (2, 0), 1, (1, 0))

    def end_pair(self):
        self.arrived(7, (2, 1), 0, (-1, 0))
        self.arrived(8, (2, 1), 1, (1, 0))

    def drain(self):
        for label, block, half, to in self.sent:
            self._copy(label, self.slot(*self._at(*block), half), *to).wait_send()


def bc_row(x, k):
    return jnp.broadcast_to(x[k : k + 1, :], (8, NB))


def bc_col(x, j):
    return jnp.broadcast_to(x[:, j : j + 1], (8, NB))


def inverse_factor(block):
    groups = NB // 8
    lane = lax.broadcasted_iota(jnp.int32, (8, NB), 1)
    sub = lax.broadcasted_iota(jnp.int32, (8, NB), 0)
    s = [block[8 * g : 8 * g + 8, :] for g in range(groups)]
    y = [jnp.where(lane == sub + 8 * g, 1.0, 0.0) for g in range(groups)]
    out = []
    for g0 in range(groups):
        top, inv = s[g0], y[g0]
        pivots = [bc_col(top, 8 * g0 + k) for k in range(8)]
        below = {g: [bc_col(s[g], 8 * g0 + k) for k in range(8)] for g in range(g0 + 1, groups)}
        scale = jnp.zeros((8, NB), jnp.float32)
        done = jnp.zeros((8, NB), jnp.float32)
        for k in range(8):
            pivot = bc_row(pivots[k], k)
            reciprocal = 1.0 / pivot
            here = sub == k
            f = jnp.where(here, 0.0, pivots[k] * reciprocal)
            scale = jnp.where(here, reciprocal, scale)
            done = jnp.where(here, inv * lax.rsqrt(pivot), done)
            for m in range(k + 1, 8):
                pivots[m] = pivots[m] - f * bc_row(pivots[m], k)
            top = top - f * bc_row(top, k)
            inv = inv - f * bc_row(inv, k)
        out.append(done)
        if g0 + 1 < groups:
            top, inv = top * scale, inv * scale
            tops = [bc_row(top, k) for k in range(8)]
            invs = [bc_row(inv, k) for k in range(8)]
            for g in range(g0 + 1, groups):
                t = [below[g][k] * tops[k] for k in range(8)]
                v = [below[g][k] * invs[k] for k in range(8)]
                while len(t) > 1:
                    t = [t[i] + t[i + 1] for i in range(0, len(t), 2)]
                    v = [v[i] + v[i + 1] for i in range(0, len(v), 2)]
                s[g] = s[g] - t[0]
                y[g] = y[g] - v[0]
    return jnp.concatenate(out, axis=0)


def whole_kernel(
    m_ref, mt_ref, result, out_ref,
    left, right, b1t, stage, a_ref, sq_ref, sh_ref, sl_ref, linv_ref, xh_ref, xl_ref,
    send, recv, swap_send, swap_recv, one_send, one_recv, local, written,
):
    row, col = lax.axis_index("row"), lax.axis_index("col")
    x, yh = lax.div(row, 2), lax.rem(row, 2)
    core, q = lax.rem(col, 2), lax.div(col, 2)
    yl, z = lax.div(q, 4), lax.rem(q, 4)
    depth, width = m_ref.shape
    height = 2 * width
    piece = SPAN // 2
    other = (row, q * 2 + 1 - core)

    def over_row(u, v):
        return (2 * u + v, col)

    def over_col(u, v):
        return (row, (4 * v + u) * 2 + core)

    def part(start, size, half):
        if half is None:
            return pl.ds(pl.multiple_of(start, 128), size)
        return pl.ds(pl.multiple_of(start + half * (size // 2), 128), size // 2)

    def right_slot(u, v, half):
        return right.at[2 * u + v, part(0, depth, half), :]

    def flip(a, b):
        return a + b - 2 * a * b

    r2, r1 = lax.div(x, 2), lax.rem(x, 2)

    def crossed(u, v):
        return 4 * flip(r2, v) + 2 * flip(r1, lax.div(u, 2)) + flip(yh, lax.rem(u, 2))

    cross = crossed(z, yl)
    blocks = {(du, dv): crossed(lax.rem(z + du + 4, 4), yl if dv == 0 else 1 - yl)
              for du in (-1, 0, 1, 2) for dv in (0, 1)}

    def left_slot(u, v, half, side=core):
        return left.at[crossed(u, v), part(side * width, width, half), :]

    def b1_slot(u, v, half, side=core):
        return b1t.at[2 * u + v, part(side * piece, piece, half), :]

    r_stream = Stream(0, send, recv, right_slot, over_row, x, yh)
    b_stream = Stream(1, send, recv, b1_slot, over_row, x, yh)
    l_stream = Stream(2, send, recv, left_slot, over_col, z, yl)
    order = ((0, 0), (0, 1), (-1, 0), (1, 0), (-1, 1), (1, 1), (2, 0), (2, 1))
    swaps = []

    def swap_copy(base, number, ref):
        place = base + number + l_stream.zero
        return pltpu.make_async_remote_copy(
            src_ref=ref, dst_ref=ref,
            send_sem=swap_send.at[place], recv_sem=swap_recv.at[place],
            device_id=other, device_id_type=MESH,
        )

    def swap_out(base, number):
        stream, slot = (b_stream, b1_slot) if base == 8 else (l_stream, left_slot)
        return swap_copy(base, number, slot(*stream._at(*order[number]), None))

    def swap(base, number):
        swap_out(base, number).start()
        swaps.append((base, number))

    def swapped(base, number):
        stream, slot = (b_stream, b1_slot) if base == 8 else (l_stream, left_slot)
        theirs = slot(*stream._at(*order[number]), None, 1 - core)
        swap_copy(base, number, theirs).wait_recv()

    def single(number, ref, target, place=None):
        return pltpu.make_async_remote_copy(
            src_ref=ref, dst_ref=ref if place is None else place,
            send_sem=one_send.at[number], recv_sem=one_recv.at[number],
            device_id=target, device_id_type=MESH,
        )

    own_right = pltpu.make_async_copy(m_ref, right.at[row], local.at[0])
    own_right.start()

    barrier = pltpu.get_barrier_semaphore()
    inside, across = (row, 2 * cross + core), (cross, col)
    friends = [
        over_row(lax.rem(x + 1, 4), yh), over_row(lax.rem(x + 3, 4), yh), over_row(x, 1 - yh),
        over_col(lax.rem(z + 1, 4), yl), over_col(lax.rem(z + 3, 4), yl), over_col(z, 1 - yl),
        other,
    ]
    for friend in friends:
        pl.semaphore_signal(barrier, inc=1, device_id=friend, device_id_type=MESH)

    moves_in, moves_across = row != 0, q != 0
    for moves, friend in ((moves_in, inside), (moves_across, across)):
        @pl.when(moves)
        def _(friend=friend):
            pl.semaphore_signal(barrier, inc=1, device_id=friend, device_id_type=MESH)

    for one in (0, 1):
        for two in (0, 1):
            here = jnp.logical_and(
                moves_in if one else row == 0, moves_across if two else q == 0
            )

            @pl.when(here)
            def _(count=len(friends) + one + two):
                pl.semaphore_wait(barrier, count)

    def mine(h):
        return part(core * width, width, h)

    def along(h):
        at = part(0, width, h)
        return single(10 + h, mt_ref.at[at, :], inside, stage.at[at, :])

    def over(h, slot):
        return single(12 + h, stage.at[part(0, width, h), :], across, left.at[slot, mine(h), :])

    def still(h):
        return pltpu.make_async_copy(
            stage.at[part(0, width, h), :], left.at[cross, mine(h), :], local.at[3 + h]
        )

    @pl.when(moves_in)
    def _():
        along(0).start()
        along(1).start()

    @pl.when(row == 0)
    def _():
        pltpu.make_async_copy(mt_ref, stage, local.at[1]).start()

    seed = jnp.logical_and(yl == 0, z == 0)
    spare = b1t.at[row, pl.ds(piece, width - piece), :]
    low = b1t.at[row, pl.ds(0, piece), :]
    high = b1t.at[row, pl.ds(width, SPAN - width), :]
    chunk = [b1_slot(x, yh, 0), b1_slot(x, yh, 1)]

    @pl.when(jnp.logical_and(seed, core == 0))
    def _():
        single(1, mt_ref.at[pl.ds(piece, width - piece), :], other, spare).start()
        copy = pltpu.make_async_copy(mt_ref.at[pl.ds(0, piece), :], low, local.at[2])
        copy.start()
        copy.wait()

    @pl.when(jnp.logical_and(seed, core == 1))
    def _():
        copy = pltpu.make_async_copy(mt_ref.at[pl.ds(0, SPAN - width), :], high, local.at[2])
        copy.start()
        copy.wait()
        single(1, spare, other).wait_recv()

    def down(h):
        single(4 + h, chunk[h], over_col(1, yl)).start()

    def up(h):
        single(6 + h, chunk[h], over_col(3, yl)).start()

    @pl.when(seed)
    def _():
        for h in range(2):
            single(2 + h, chunk[h], over_col(0, 1)).start()
            down(h)
            up(1 - h)

    own_right.wait()
    r_stream.push(0, (0, 0), None, (0, 1))
    r_stream.push(1, (0, 0), None, (1, 0))
    r_stream.push(2, (0, 0), None, (-1, 0))

    @pl.when(jnp.logical_and(z == 0, yl == 1))
    def _():
        for h in range(2):
            single(2 + h, chunk[h], over_col(0, 0)).wait_recv()
            down(h)
            up(h)

    @pl.when(z == 1)
    def _():
        single(4, chunk[0], over_col(0, yl)).wait_recv()
        single(8, chunk[0], over_col(2, yl)).start()
        single(5, chunk[1], over_col(0, yl)).wait_recv()

    @pl.when(z == 3)
    def _():
        single(7, chunk[1], over_col(0, yl)).wait_recv()
        single(9, chunk[1], over_col(2, yl)).start()
        single(6, chunk[0], over_col(0, yl)).wait_recv()

    @pl.when(row == 0)
    def _():
        pltpu.make_async_copy(mt_ref, stage, local.at[1]).wait()

    for h in range(2):
        @pl.when(moves_in)
        def _(h=h):
            along(h).wait_recv()

        @pl.when(moves_across)
        def _(h=h):
            over(h, row).start()

        @pl.when(q == 0)
        def _(h=h):
            still(h).start()

    @pl.when(z == 2)
    def _():
        single(8, chunk[0], over_col(1, yl)).wait_recv()
        single(9, chunk[1], over_col(3, yl)).wait_recv()

    b_stream.send_own()
    swap(8, 0)

    rows = 512

    def at_tile(tile):
        return pl.ds(pl.multiple_of(tile * rows, rows), rows)

    def gram(number):
        swapped(8, number)
        uu, vv = b_stream._at(*order[number])
        k = 2 * uu + vv

        def over_span(tile, carry):
            value = nt(b1t[k, at_tile(tile), :], b1t[k])
            if number == 0:
                a_ref[at_tile(tile), :] = value
            else:
                a_ref[at_tile(tile), :] += value
            return carry

        lax.fori_loop(0, SPAN // rows, over_span, 0)

    b_stream.send_pair()
    swap(8, 1)
    for h in range(2):
        @pl.when(moves_across)
        def _(h=h):
            over(h, cross).wait_recv()

        @pl.when(q == 0)
        def _(h=h):
            still(h).wait()

    l_stream.send_own()
    swap(0, 0)
    b_stream.relay_own()
    swap(8, 2)
    swap(8, 3)
    gram(0)
    gram(1)
    b_stream.relay_pair()
    swap(8, 4)
    swap(8, 5)
    r_stream.relay_own()
    r_stream.send_pair()
    gram(2)
    gram(3)
    l_stream.send_pair()
    swap(0, 1)
    l_stream.relay_own()
    swap(0, 2)
    swap(0, 3)
    b_stream.end_own()
    swap(8, 6)
    gram(4)
    gram(5)
    b_stream.end_pair()
    swap(8, 7)
    gram(6)
    gram(7)

    eye = jnp.where(
        lax.broadcasted_iota(jnp.int32, (NB, NB), 0) == lax.broadcasted_iota(jnp.int32, (NB, NB), 1),
        1.0, 0.0,
    )
    for b in range(BLOCKS):
        at = slice(b * NB, (b + 1) * NB)
        a_ref[at, at] += eye
    linv_ref[...] = jnp.zeros_like(linv_ref)
    tall = 256

    right_order = [2 * r_stream._at(*o)[0] + r_stream._at(*o)[1] for o in order]
    left_order = [blocks[o] for o in order]

    def choose(b, values):
        value = values[0]
        for i in range(1, BLOCKS):
            value = lax.select(b == i, values[i], value)
        return value

    sq_ref[...] = jnp.zeros_like(sq_ref)
    out_ref[...] = jnp.zeros_like(out_ref)
    half_rows = part(core * width, width, None)

    def factor_step(b, carry):
        r_stream.zero = l_stream.zero = b * 0

        @pl.when(b == 2)
        def _():
            l_stream.relay_pair()
            swap(0, 4)
            swap(0, 5)

        @pl.when(b == 3)
        def _():
            r_stream.relay_pair()

        @pl.when(b == 6)
        def _():
            r_stream.end_own()
            l_stream.end_own()
            swap(0, 6)

        @pl.when(b == 7)
        def _():
            r_stream.end_pair()
            l_stream.end_pair()
            swap(0, 7)

        at = pl.ds(pl.multiple_of(b * NB, NB), NB)
        y = inverse_factor(a_ref[at, at])
        linv_ref[at, at] = y
        kr, kl = choose(b, right_order), choose(b, left_order)
        sq_ref[...] += nn(b1t[kr], right[kr])
        lhs = left[kl, half_rows, :]
        out_ref[0:width, :] += nt(lhs, b1t[kl, 0:width, :])
        out_ref[width:height, 0 : SPAN - width] += nt(lhs, b1t[kl, width:SPAN, :])
        below = lax.broadcasted_iota(jnp.int32, (SPAN, NB), 0) >= (b + 1) * NB
        panel = three(nt, split(a_ref[:, at]), split(y))
        panel = jnp.where(below, panel, 0.0)
        a_ref[:, at] = panel
        xh_ref[:, 0:NB], xl_ref[:, 0:NB] = split(panel)

        def update(tile, c):
            part_rows = pl.ds(pl.multiple_of(tile * tall, tall), tall)
            a_ref[part_rows, :] -= three(
                nt,
                (xh_ref[part_rows, 0:NB], xl_ref[part_rows, 0:NB]),
                (xh_ref[:, 0:NB], xl_ref[:, 0:NB]),
            )
            return c

        lax.fori_loop((b + 1) // 2, SPAN // tall, update, 0)

        return carry

    lax.fori_loop(0, BLOCKS, factor_step, 0)
    r_stream.zero = l_stream.zero = 0

    first = row * height + core * width
    for t in range(width // tall):
        to = pl.ds(pl.multiple_of(core * width + t * tall, tall), tall)
        for base, lo, hi in ((0, 0, width), (width, width, SPAN)):
            shape = (tall, hi - lo)
            srow = first + t * tall + lax.broadcasted_iota(jnp.int32, shape, 0)
            scol = lo + lax.broadcasted_iota(jnp.int32, shape, 1)
            strip = out_ref[base + t * tall : base + (t + 1) * tall, 0 : hi - lo]
            strip += jnp.where(srow == scol, 1.0, 0.0)
            sh_ref[to, lo:hi], sl_ref[to, lo:hi] = split(strip)

    size = NB
    while size < SPAN:
        for lo in range(0, SPAN, 2 * size):
            one, two = slice(lo, lo + size), slice(lo + size, lo + 2 * size)
            inner = three(nn, split(a_ref[two, one]), split(linv_ref[one, one]))
            linv_ref[two, one] = -three(nn, split(linv_ref[two, two]), split(inner))
        size *= 2

    def strips(side):
        at = part(side * width, width, None)
        return [single(14 + i, ref.at[at, :], other) for i, ref in enumerate((sh_ref, sl_ref))]

    for copy in strips(core):
        copy.start()

    cols = col * width + lax.broadcasted_iota(jnp.int32, (tall, width), 1)
    for b in range(SPAN // tall):
        at = slice(b * tall, (b + 1) * tall)
        upto = slice(0, (b + 1) * tall)
        solved = three(nn, split(linv_ref[at, upto]), split(sq_ref[upto, :]))
        unit = jnp.where(b * tall + lax.broadcasted_iota(jnp.int32, (tall, width), 0) == cols, 1.0, 0.0)
        xh_ref[at, :], xl_ref[at, :] = split(jnp.where(cols < SPAN, unit, solved))
    for b in range(SPAN // tall):
        at = slice(b * tall, (b + 1) * tall)
        onward = slice(b * tall, SPAN)
        sq_ref[at, :] = three(tn, split(linv_ref[onward, at]), (xh_ref[onward, :], xl_ref[onward, :]))
    for b in range(SPAN // tall):
        at = slice(b * tall, (b + 1) * tall)
        xh_ref[at, :], xl_ref[at, :] = split(sq_ref[at, :])

    for number in range(8):
        swapped(0, number)

    def over_rows(t, carry):
        at = pl.ds(pl.multiple_of(t * tall, tall), tall)
        value = nn(left[0, at, :], right[0])
        for i in range(1, 8):
            value += nn(left[i, at, :], right[i])
        out_ref[at, :] = value
        return carry

    lax.fori_loop(0, height // tall, over_rows, 0)
    for copy in strips(1 - core):
        copy.wait_recv()

    def finish(t, carry):
        at = pl.ds(pl.multiple_of(t * tall, tall), tall)
        first = row * height + t * tall
        grow = first + lax.broadcasted_iota(jnp.int32, (tall, width), 0)
        gcol = col * width + lax.broadcasted_iota(jnp.int32, (tall, width), 1)
        value = nn(sh_ref[at, :], xh_ref[...]) + nn(sh_ref[at, :], xl_ref[...])
        system = out_ref[at, :] + jnp.where(grow == gcol, 1.0, 0.0)
        lead = jnp.where(grow >= gcol, value, 0.0)
        rest = jnp.where(grow < SPAN, 0.0, system - value)
        out_ref[at, :] = jnp.where(gcol < SPAN, lead, rest)

        @pl.when(col < 2)
        def _():
            low = nn(sl_ref[at, :], xh_ref[...])
            keep = jnp.logical_and(gcol < SPAN, grow >= gcol)
            out_ref[at, :] += jnp.where(keep, low, 0.0)

        pltpu.make_async_copy(out_ref.at[at, :], result.at[at, :], written.at[t]).start()
        return carry

    lax.fori_loop(0, height // tall, finish, 0)

    def landed(t, carry):
        at = pl.ds(pl.multiple_of(t * tall, tall), tall)
        pltpu.make_async_copy(out_ref.at[at, :], result.at[at, :], written.at[t]).wait()
        return carry

    for stream in (r_stream, b_stream, l_stream):
        stream.drain()
    for base, number in swaps:
        swap_out(base, number).wait_send()

    for copy in strips(core):
        copy.wait_send()

    for h in range(2):
        @pl.when(moves_in)
        def _(h=h):
            along(h).wait_send()

        @pl.when(moves_across)
        def _(h=h):
            over(h, row).wait_send()

    @pl.when(jnp.logical_and(seed, core == 0))
    def _():
        single(1, mt_ref.at[pl.ds(piece, width - piece), :], other, spare).wait_send()

    @pl.when(seed)
    def _():
        for h in range(2):
            single(2 + h, chunk[h], over_col(0, 1)).wait_send()

    @pl.when(z == 0)
    def _():
        for h in range(2):
            single(4 + h, chunk[h], over_col(1, yl)).wait_send()
            single(6 + h, chunk[h], over_col(3, yl)).wait_send()

    @pl.when(z == 1)
    def _():
        single(8, chunk[0], over_col(2, yl)).wait_send()

    @pl.when(z == 3)
    def _():
        single(9, chunk[1], over_col(2, yl)).wait_send()

    lax.fori_loop(0, height // tall, landed, 0)


def whole(masked, transposed):
    depth, width = masked.shape
    height = 2 * width
    f32, bf16 = jnp.float32, jnp.bfloat16
    dma = pltpu.SemaphoreType.DMA
    hbm = pl.BlockSpec(memory_space=pl.ANY)
    return pl.pallas_call(
        whole_kernel,
        out_shape=jax.ShapeDtypeStruct((height, width), f32),
        in_specs=[hbm, hbm],
        out_specs=hbm,
        scratch_shapes=[
            pltpu.VMEM((height, width), f32),
            pltpu.VMEM((8, height, depth), bf16),
            pltpu.VMEM((8, depth, width), bf16),
            pltpu.VMEM((8, SPAN, depth), bf16),
            pltpu.VMEM((width, depth), bf16),
            pltpu.VMEM((SPAN, SPAN), f32),
            pltpu.VMEM((SPAN, width), f32),
            pltpu.VMEM((height, SPAN), bf16),
            pltpu.VMEM((height, SPAN), bf16),
            pltpu.VMEM((SPAN, SPAN), f32),
            pltpu.VMEM((SPAN, width), bf16),
            pltpu.VMEM((SPAN, width), bf16),
            dma((3, 9)), dma((3, 9)),
            dma((16,)), dma((16,)),
            dma((16,)), dma((16,)),
            dma((5,)),
            dma((height // TILE,)),
        ],
        compiler_params=pltpu.CompilerParams(
            collective_id=0, has_side_effects=True, vmem_limit_bytes=VMEM_LIMIT
        ),
        name="whole",
    )(masked, transposed)


def expand_tiles(blocks):
    return jnp.repeat(jnp.repeat(blocks, TILE, axis=0), TILE, axis=1)


def on_device(b_values, tile_mask):
    row_index = lax.axis_index("row")
    col_index = lax.axis_index("col")
    depth, width = b_values.shape
    occupancy = lax.dynamic_slice(
        tile_mask,
        (row_index * (depth // TILE), col_index * (width // TILE)),
        (depth // TILE, width // TILE),
    )
    masked = b_values * expand_tiles(occupancy).astype(jnp.bfloat16)
    return whole(masked, masked.T)


def solution(mesh):
    return jax.shard_map(
        on_device,
        mesh=mesh,
        in_specs=(P("row", "col"), P()),
        out_specs=P("row", "col"),
        check_vma=False,
    )
```

```python
import functools

import jax
import jax.numpy as jnp
from jax import lax
from jax.experimental import pallas as pl
from jax.experimental.pallas import tpu as pltpu
from jax.sharding import PartitionSpec as P

TILE = 256
PANEL = 512
SPAN = 2 * PANEL
NB = 128
BLOCKS = SPAN // NB
MESH = pl.DeviceIdType.MESH
VMEM_LIMIT = 66_000_000


def nn(a, b):
    return lax.dot_general(a, b, (((1,), (0,)), ((), ())), preferred_element_type=jnp.float32)


def nt(a, b):
    return lax.dot_general(a, b, (((1,), (1,)), ((), ())), preferred_element_type=jnp.float32)


def tn(a, b):
    return lax.dot_general(a, b, (((0,), (0,)), ((), ())), preferred_element_type=jnp.float32)


def split(value):
    high = value.astype(jnp.bfloat16)
    return high, (value - high.astype(jnp.float32)).astype(jnp.bfloat16)


def three(dot, a, b):
    (ah, al), (bh, bl) = a, b
    return dot(ah, bh) + (dot(al, bh) + dot(ah, bl))


class Stream:
    def __init__(self, index, send, recv, slot, device, u, v):
        self.index, self.send, self.recv = index, send, recv
        self.slot, self.device, self.u, self.v = slot, device, u, v
        self.sent = []
        self.ring = {du: lax.rem(u + du + 4, 4) for du in (-1, 0, 1, 2)}
        self.pair = {0: v, 1: 1 - v}
        self.zero = 0

    def _at(self, du, dv):
        return self.ring[du], self.pair[dv]

    def _copy(self, label, ref, du, dv):
        uu, vv = self._at(du, dv)
        return pltpu.make_async_remote_copy(
            src_ref=ref,
            dst_ref=ref,
            send_sem=self.send.at[self.index + self.zero, label + self.zero],
            recv_sem=self.recv.at[self.index + self.zero, label + self.zero],
            device_id=self.device(uu, vv),
            device_id_type=MESH,
        )

    def push(self, label, block, half, to):
        copy = self._copy(label, self.slot(*self._at(*block), half), *to)
        copy.start()
        self.sent.append((label, block, half, to))

    def arrived(self, label, block, half, source):
        self._copy(label, self.slot(*self._at(*block), half), *source).wait_recv()

    def send_own(self):
        self.push(0, (0, 0), None, (0, 1))
        self.push(1, (0, 0), None, (1, 0))
        self.push(2, (0, 0), None, (-1, 0))

    def send_pair(self):
        self.arrived(0, (0, 1), None, (0, 1))
        self.push(3, (0, 1), None, (1, 0))
        self.push(4, (0, 1), None, (-1, 0))

    def relay_own(self):
        self.arrived(1, (-1, 0), None, (-1, 0))
        self.push(5, (-1, 0), 0, (1, 0))
        self.arrived(2, (1, 0), None, (1, 0))
        self.push(6, (1, 0), 1, (-1, 0))

    def relay_pair(self):
        self.arrived(3, (-1, 1), None, (-1, 0))
        self.push(7, (-1, 1), 0, (1, 0))
        self.arrived(4, (1, 1), None, (1, 0))
        self.push(8, (1, 1), 1, (-1, 0))

    def end_own(self):
        self.arrived(5, (2, 0), 0, (-1, 0))
        self.arrived(6, (2, 0), 1, (1, 0))

    def end_pair(self):
        self.arrived(7, (2, 1), 0, (-1, 0))
        self.arrived(8, (2, 1), 1, (1, 0))

    def drain(self):
        for label, block, half, to in self.sent:
            self._copy(label, self.slot(*self._at(*block), half), *to).wait_send()


def bc_row(x, k):
    return jnp.broadcast_to(x[k : k + 1, :], (8, NB))


def bc_col(x, j):
    return jnp.broadcast_to(x[:, j : j + 1], (8, NB))


def inverse_factor(block):
    groups = NB // 8
    lane = lax.broadcasted_iota(jnp.int32, (8, NB), 1)
    sub = lax.broadcasted_iota(jnp.int32, (8, NB), 0)
    s = [block[8 * g : 8 * g + 8, :] for g in range(groups)]
    y = [jnp.where(lane == sub + 8 * g, 1.0, 0.0) for g in range(groups)]
    out = []
    for g0 in range(groups):
        top, inv = s[g0], y[g0]
        pivots = [bc_col(top, 8 * g0 + k) for k in range(8)]
        below = {g: [bc_col(s[g], 8 * g0 + k) for k in range(8)] for g in range(g0 + 1, groups)}
        scale = jnp.zeros((8, NB), jnp.float32)
        done = jnp.zeros((8, NB), jnp.float32)
        for k in range(8):
            pivot = bc_row(pivots[k], k)
            reciprocal = 1.0 / pivot
            here = sub == k
            f = jnp.where(here, 0.0, pivots[k] * reciprocal)
            scale = jnp.where(here, reciprocal, scale)
            done = jnp.where(here, inv * lax.rsqrt(pivot), done)
            for m in range(k + 1, 8):
                pivots[m] = pivots[m] - f * bc_row(pivots[m], k)
            top = top - f * bc_row(top, k)
            inv = inv - f * bc_row(inv, k)
        out.append(done)
        if g0 + 1 < groups:
            top, inv = top * scale, inv * scale
            tops = [bc_row(top, k) for k in range(8)]
            invs = [bc_row(inv, k) for k in range(8)]
            for g in range(g0 + 1, groups):
                t = [below[g][k] * tops[k] for k in range(8)]
                v = [below[g][k] * invs[k] for k in range(8)]
                while len(t) > 1:
                    t = [t[i] + t[i + 1] for i in range(0, len(t), 2)]
                    v = [v[i] + v[i + 1] for i in range(0, len(v), 2)]
                s[g] = s[g] - t[0]
                y[g] = y[g] - v[0]
    return jnp.concatenate(out, axis=0)


def whole_kernel(
    m_ref, mt_ref, result, out_ref,
    left, right, b1t, stage, a_ref, sq_ref, sh_ref, sl_ref, linv_ref, xh_ref, xl_ref,
    send, recv, swap_send, swap_recv, one_send, one_recv, local, written,
):
    row, col = lax.axis_index("row"), lax.axis_index("col")
    x, yh = lax.div(row, 2), lax.rem(row, 2)
    core, q = lax.rem(col, 2), lax.div(col, 2)
    yl, z = lax.div(q, 4), lax.rem(q, 4)
    depth, width = m_ref.shape
    height = 2 * width
    piece = SPAN // 2
    other = (row, q * 2 + 1 - core)

    def over_row(u, v):
        return (2 * u + v, col)

    def over_col(u, v):
        return (row, (4 * v + u) * 2 + core)

    def part(start, size, half):
        if half is None:
            return pl.ds(pl.multiple_of(start, 128), size)
        return pl.ds(pl.multiple_of(start + half * (size // 2), 128), size // 2)

    def right_slot(u, v, half):
        return right.at[2 * u + v, part(0, depth, half), :]

    def flip(a, b):
        return a + b - 2 * a * b

    r2, r1 = lax.div(x, 2), lax.rem(x, 2)

    def crossed(u, v):
        return 4 * flip(r2, v) + 2 * flip(r1, lax.div(u, 2)) + flip(yh, lax.rem(u, 2))

    cross = crossed(z, yl)
    blocks = {(du, dv): crossed(lax.rem(z + du + 4, 4), yl if dv == 0 else 1 - yl)
              for du in (-1, 0, 1, 2) for dv in (0, 1)}

    def left_slot(u, v, half, side=core):
        return left.at[crossed(u, v), part(side * width, width, half), :]

    def b1_slot(u, v, half, side=core):
        return b1t.at[2 * u + v, part(side * piece, piece, half), :]

    r_stream = Stream(0, send, recv, right_slot, over_row, x, yh)
    b_stream = Stream(1, send, recv, b1_slot, over_row, x, yh)
    l_stream = Stream(2, send, recv, left_slot, over_col, z, yl)
    order = ((0, 0), (0, 1), (-1, 0), (1, 0), (-1, 1), (1, 1), (2, 0), (2, 1))
    swaps = []

    def swap_copy(base, number, ref):
        place = base + number + l_stream.zero
        return pltpu.make_async_remote_copy(
            src_ref=ref, dst_ref=ref,
            send_sem=swap_send.at[place], recv_sem=swap_recv.at[place],
            device_id=other, device_id_type=MESH,
        )

    def swap_out(base, number):
        stream, slot = (b_stream, b1_slot) if base == 8 else (l_stream, left_slot)
        return swap_copy(base, number, slot(*stream._at(*order[number]), None))

    def swap(base, number):
        swap_out(base, number).start()
        swaps.append((base, number))

    def swapped(base, number):
        stream, slot = (b_stream, b1_slot) if base == 8 else (l_stream, left_slot)
        theirs = slot(*stream._at(*order[number]), None, 1 - core)
        swap_copy(base, number, theirs).wait_recv()

    def single(number, ref, target, place=None):
        return pltpu.make_async_remote_copy(
            src_ref=ref, dst_ref=ref if place is None else place,
            send_sem=one_send.at[number], recv_sem=one_recv.at[number],
            device_id=target, device_id_type=MESH,
        )

    own_right = pltpu.make_async_copy(m_ref, right.at[row], local.at[0])
    own_right.start()

    barrier = pltpu.get_barrier_semaphore()
    inside, across = (row, 2 * cross + core), (cross, col)
    friends = [
        over_row(lax.rem(x + 1, 4), yh), over_row(lax.rem(x + 3, 4), yh), over_row(x, 1 - yh),
        over_col(lax.rem(z + 1, 4), yl), over_col(lax.rem(z + 3, 4), yl), over_col(z, 1 - yl),
        other,
    ]
    for friend in friends:
        pl.semaphore_signal(barrier, inc=1, device_id=friend, device_id_type=MESH)

    moves_in, moves_across = row != 0, q != 0
    for moves, friend in ((moves_in, inside), (moves_across, across)):
        @pl.when(moves)
        def _(friend=friend):
            pl.semaphore_signal(barrier, inc=1, device_id=friend, device_id_type=MESH)

    for one in (0, 1):
        for two in (0, 1):
            here = jnp.logical_and(
                moves_in if one else row == 0, moves_across if two else q == 0
            )

            @pl.when(here)
            def _(count=len(friends) + one + two):
                pl.semaphore_wait(barrier, count)

    def mine(h):
        return part(core * width, width, h)

    def along(h):
        at = part(0, width, h)
        return single(10 + h, mt_ref.at[at, :], inside, stage.at[at, :])

    def over(h, slot):
        return single(12 + h, stage.at[part(0, width, h), :], across, left.at[slot, mine(h), :])

    def still(h):
        return pltpu.make_async_copy(
            stage.at[part(0, width, h), :], left.at[cross, mine(h), :], local.at[3 + h]
        )

    @pl.when(moves_in)
    def _():
        along(0).start()
        along(1).start()

    @pl.when(row == 0)
    def _():
        pltpu.make_async_copy(mt_ref, stage, local.at[1]).start()

    seed = jnp.logical_and(yl == 0, z == 0)
    spare = b1t.at[row, pl.ds(piece, width - piece), :]
    low = b1t.at[row, pl.ds(0, piece), :]
    high = b1t.at[row, pl.ds(width, SPAN - width), :]
    chunk = [b1_slot(x, yh, 0), b1_slot(x, yh, 1)]

    @pl.when(jnp.logical_and(seed, core == 0))
    def _():
        single(1, mt_ref.at[pl.ds(piece, width - piece), :], other, spare).start()
        copy = pltpu.make_async_copy(mt_ref.at[pl.ds(0, piece), :], low, local.at[2])
        copy.start()
        copy.wait()

    @pl.when(jnp.logical_and(seed, core == 1))
    def _():
        copy = pltpu.make_async_copy(mt_ref.at[pl.ds(0, SPAN - width), :], high, local.at[2])
        copy.start()
        copy.wait()
        single(1, spare, other).wait_recv()

    def down(h):
        single(4 + h, chunk[h], over_col(1, yl)).start()

    def up(h):
        single(6 + h, chunk[h], over_col(3, yl)).start()

    @pl.when(seed)
    def _():
        for h in range(2):
            single(2 + h, chunk[h], over_col(0, 1)).start()
            down(h)
            up(1 - h)

    own_right.wait()
    r_stream.push(0, (0, 0), None, (0, 1))
    r_stream.push(1, (0, 0), None, (1, 0))
    r_stream.push(2, (0, 0), None, (-1, 0))

    @pl.when(jnp.logical_and(z == 0, yl == 1))
    def _():
        for h in range(2):
            single(2 + h, chunk[h], over_col(0, 0)).wait_recv()
            down(h)
            up(h)

    @pl.when(z == 1)
    def _():
        single(4, chunk[0], over_col(0, yl)).wait_recv()
        single(8, chunk[0], over_col(2, yl)).start()
        single(5, chunk[1], over_col(0, yl)).wait_recv()

    @pl.when(z == 3)
    def _():
        single(7, chunk[1], over_col(0, yl)).wait_recv()
        single(9, chunk[1], over_col(2, yl)).start()
        single(6, chunk[0], over_col(0, yl)).wait_recv()

    @pl.when(row == 0)
    def _():
        pltpu.make_async_copy(mt_ref, stage, local.at[1]).wait()

    for h in range(2):
        @pl.when(moves_in)
        def _(h=h):
            along(h).wait_recv()

        @pl.when(moves_across)
        def _(h=h):
            over(h, row).start()

        @pl.when(q == 0)
        def _(h=h):
            still(h).start()

    @pl.when(z == 2)
    def _():
        single(8, chunk[0], over_col(1, yl)).wait_recv()
        single(9, chunk[1], over_col(3, yl)).wait_recv()

    b_stream.send_own()
    swap(8, 0)

    rows = 512

    def at_tile(tile):
        return pl.ds(pl.multiple_of(tile * rows, rows), rows)

    def gram(number):
        swapped(8, number)
        uu, vv = b_stream._at(*order[number])
        k = 2 * uu + vv

        def over_span(tile, carry):
            value = nt(b1t[k, at_tile(tile), :], b1t[k])
            if number == 0:
                a_ref[at_tile(tile), :] = value
            else:
                a_ref[at_tile(tile), :] += value
            return carry

        lax.fori_loop(0, SPAN // rows, over_span, 0)

    b_stream.send_pair()
    swap(8, 1)
    for h in range(2):
        @pl.when(moves_across)
        def _(h=h):
            over(h, cross).wait_recv()

        @pl.when(q == 0)
        def _(h=h):
            still(h).wait()

    l_stream.send_own()
    swap(0, 0)
    b_stream.relay_own()
    swap(8, 2)
    swap(8, 3)
    gram(0)
    gram(1)
    b_stream.relay_pair()
    swap(8, 4)
    swap(8, 5)
    r_stream.relay_own()
    r_stream.send_pair()
    gram(2)
    gram(3)
    l_stream.send_pair()
    swap(0, 1)
    l_stream.relay_own()
    swap(0, 2)
    swap(0, 3)
    b_stream.end_own()
    swap(8, 6)
    gram(4)
    gram(5)
    b_stream.end_pair()
    swap(8, 7)
    gram(6)
    gram(7)

    eye = jnp.where(
        lax.broadcasted_iota(jnp.int32, (NB, NB), 0) == lax.broadcasted_iota(jnp.int32, (NB, NB), 1),
        1.0, 0.0,
    )
    for b in range(BLOCKS):
        at = slice(b * NB, (b + 1) * NB)
        a_ref[at, at] += eye
    linv_ref[...] = jnp.zeros_like(linv_ref)
    tall = 256

    right_order = [2 * r_stream._at(*o)[0] + r_stream._at(*o)[1] for o in order]
    left_order = [blocks[o] for o in order]

    def choose(b, values):
        value = values[0]
        for i in range(1, BLOCKS):
            value = lax.select(b == i, values[i], value)
        return value

    sq_ref[...] = jnp.zeros_like(sq_ref)
    out_ref[...] = jnp.zeros_like(out_ref)
    half_rows = part(core * width, width, None)

    def factor_step(b, carry):
        r_stream.zero = l_stream.zero = b * 0

        @pl.when(b == 1)
        def _():
            l_stream.relay_pair()
            swap(0, 4)
            swap(0, 5)

        @pl.when(b == 2)
        def _():
            r_stream.relay_pair()

        @pl.when(b == 6)
        def _():
            r_stream.end_own()
            l_stream.end_own()
            swap(0, 6)

        @pl.when(b == 7)
        def _():
            r_stream.end_pair()
            l_stream.end_pair()
            swap(0, 7)

        at = pl.ds(pl.multiple_of(b * NB, NB), NB)
        y = inverse_factor(a_ref[at, at])
        linv_ref[at, at] = y
        kr, kl = choose(b, right_order), choose(b, left_order)
        sq_ref[...] += nn(b1t[kr], right[kr])
        lhs = left[kl, half_rows, :]
        out_ref[0:width, :] += nt(lhs, b1t[kl, 0:width, :])
        out_ref[width:height, 0 : SPAN - width] += nt(lhs, b1t[kl, width:SPAN, :])
        below = lax.broadcasted_iota(jnp.int32, (SPAN, NB), 0) >= (b + 1) * NB
        panel = three(nt, split(a_ref[:, at]), split(y))
        panel = jnp.where(below, panel, 0.0)
        a_ref[:, at] = panel
        xh_ref[:, 0:NB], xl_ref[:, 0:NB] = split(panel)

        def update(tile, c):
            part_rows = pl.ds(pl.multiple_of(tile * tall, tall), tall)
            a_ref[part_rows, :] -= three(
                nt,
                (xh_ref[part_rows, 0:NB], xl_ref[part_rows, 0:NB]),
                (xh_ref[:, 0:NB], xl_ref[:, 0:NB]),
            )
            return c

        lax.fori_loop((b + 1) // 2, SPAN // tall, update, 0)

        return carry

    lax.fori_loop(0, BLOCKS, factor_step, 0)
    r_stream.zero = l_stream.zero = 0

    first = row * height + core * width
    for t in range(width // tall):
        to = pl.ds(pl.multiple_of(core * width + t * tall, tall), tall)
        for base, lo, hi in ((0, 0, width), (width, width, SPAN)):
            shape = (tall, hi - lo)
            srow = first + t * tall + lax.broadcasted_iota(jnp.int32, shape, 0)
            scol = lo + lax.broadcasted_iota(jnp.int32, shape, 1)
            strip = out_ref[base + t * tall : base + (t + 1) * tall, 0 : hi - lo]
            strip += jnp.where(srow == scol, 1.0, 0.0)
            sh_ref[to, lo:hi], sl_ref[to, lo:hi] = split(strip)

    size = NB
    while size < SPAN:
        for lo in range(0, SPAN, 2 * size):
            one, two = slice(lo, lo + size), slice(lo + size, lo + 2 * size)
            inner = three(nn, split(a_ref[two, one]), split(linv_ref[one, one]))
            linv_ref[two, one] = -three(nn, split(linv_ref[two, two]), split(inner))
        size *= 2

    def strips(side):
        at = part(side * width, width, None)
        return [single(14 + i, ref.at[at, :], other) for i, ref in enumerate((sh_ref, sl_ref))]

    for copy in strips(core):
        copy.start()

    cols = col * width + lax.broadcasted_iota(jnp.int32, (tall, width), 1)
    for b in range(SPAN // tall):
        at = slice(b * tall, (b + 1) * tall)
        upto = slice(0, (b + 1) * tall)
        solved = three(nn, split(linv_ref[at, upto]), split(sq_ref[upto, :]))
        unit = jnp.where(b * tall + lax.broadcasted_iota(jnp.int32, (tall, width), 0) == cols, 1.0, 0.0)
        xh_ref[at, :], xl_ref[at, :] = split(jnp.where(cols < SPAN, unit, solved))
    for b in range(SPAN // tall):
        at = slice(b * tall, (b + 1) * tall)
        onward = slice(b * tall, SPAN)
        sq_ref[at, :] = three(tn, split(linv_ref[onward, at]), (xh_ref[onward, :], xl_ref[onward, :]))
    for b in range(SPAN // tall):
        at = slice(b * tall, (b + 1) * tall)
        xh_ref[at, :], xl_ref[at, :] = split(sq_ref[at, :])

    for number in range(8):
        swapped(0, number)

    def over_rows(t, carry):
        at = pl.ds(pl.multiple_of(t * tall, tall), tall)
        value = nn(left[0, at, :], right[0])
        for i in range(1, 8):
            value += nn(left[i, at, :], right[i])
        out_ref[at, :] = value
        return carry

    lax.fori_loop(0, height // tall, over_rows, 0)
    for copy in strips(1 - core):
        copy.wait_recv()

    def finish(t, carry):
        at = pl.ds(pl.multiple_of(t * tall, tall), tall)
        first = row * height + t * tall
        grow = first + lax.broadcasted_iota(jnp.int32, (tall, width), 0)
        gcol = col * width + lax.broadcasted_iota(jnp.int32, (tall, width), 1)
        value = nn(sh_ref[at, :], xh_ref[...]) + nn(sh_ref[at, :], xl_ref[...])
        system = out_ref[at, :] + jnp.where(grow == gcol, 1.0, 0.0)
        lead = jnp.where(grow >= gcol, value, 0.0)
        rest = jnp.where(grow < SPAN, 0.0, system - value)
        out_ref[at, :] = jnp.where(gcol < SPAN, lead, rest)

        @pl.when(col < 2)
        def _():
            low = nn(sl_ref[at, :], xh_ref[...])
            keep = jnp.logical_and(gcol < SPAN, grow >= gcol)
            out_ref[at, :] += jnp.where(keep, low, 0.0)

        pltpu.make_async_copy(out_ref.at[at, :], result.at[at, :], written.at[t]).start()
        return carry

    lax.fori_loop(0, height // tall, finish, 0)

    def landed(t, carry):
        at = pl.ds(pl.multiple_of(t * tall, tall), tall)
        pltpu.make_async_copy(out_ref.at[at, :], result.at[at, :], written.at[t]).wait()
        return carry

    for stream in (r_stream, b_stream, l_stream):
        stream.drain()
    for base, number in swaps:
        swap_out(base, number).wait_send()

    for copy in strips(core):
        copy.wait_send()

    for h in range(2):
        @pl.when(moves_in)
        def _(h=h):
            along(h).wait_send()

        @pl.when(moves_across)
        def _(h=h):
            over(h, row).wait_send()

    @pl.when(jnp.logical_and(seed, core == 0))
    def _():
        single(1, mt_ref.at[pl.ds(piece, width - piece), :], other, spare).wait_send()

    @pl.when(seed)
    def _():
        for h in range(2):
            single(2 + h, chunk[h], over_col(0, 1)).wait_send()

    @pl.when(z == 0)
    def _():
        for h in range(2):
            single(4 + h, chunk[h], over_col(1, yl)).wait_send()
            single(6 + h, chunk[h], over_col(3, yl)).wait_send()

    @pl.when(z == 1)
    def _():
        single(8, chunk[0], over_col(2, yl)).wait_send()

    @pl.when(z == 3)
    def _():
        single(9, chunk[1], over_col(2, yl)).wait_send()

    lax.fori_loop(0, height // tall, landed, 0)


def whole(masked, transposed):
    depth, width = masked.shape
    height = 2 * width
    f32, bf16 = jnp.float32, jnp.bfloat16
    dma = pltpu.SemaphoreType.DMA
    hbm = pl.BlockSpec(memory_space=pl.ANY)
    return pl.pallas_call(
        whole_kernel,
        out_shape=jax.ShapeDtypeStruct((height, width), f32),
        in_specs=[hbm, hbm],
        out_specs=hbm,
        scratch_shapes=[
            pltpu.VMEM((height, width), f32),
            pltpu.VMEM((8, height, depth), bf16),
            pltpu.VMEM((8, depth, width), bf16),
            pltpu.VMEM((8, SPAN, depth), bf16),
            pltpu.VMEM((width, depth), bf16),
            pltpu.VMEM((SPAN, SPAN), f32),
            pltpu.VMEM((SPAN, width), f32),
            pltpu.VMEM((height, SPAN), bf16),
            pltpu.VMEM((height, SPAN), bf16),
            pltpu.VMEM((SPAN, SPAN), f32),
            pltpu.VMEM((SPAN, width), bf16),
            pltpu.VMEM((SPAN, width), bf16),
            dma((3, 9)), dma((3, 9)),
            dma((16,)), dma((16,)),
            dma((16,)), dma((16,)),
            dma((5,)),
            dma((height // TILE,)),
        ],
        compiler_params=pltpu.CompilerParams(
            collective_id=0, has_side_effects=True, vmem_limit_bytes=VMEM_LIMIT
        ),
        name="whole",
    )(masked, transposed)


def expand_tiles(blocks):
    return jnp.repeat(jnp.repeat(blocks, TILE, axis=0), TILE, axis=1)


def on_device(b_values, tile_mask):
    row_index = lax.axis_index("row")
    col_index = lax.axis_index("col")
    depth, width = b_values.shape
    occupancy = lax.dynamic_slice(
        tile_mask,
        (row_index * (depth // TILE), col_index * (width // TILE)),
        (depth // TILE, width // TILE),
    )
    masked = b_values * expand_tiles(occupancy).astype(jnp.bfloat16)
    return whole(masked, masked.T)


def solution(mesh):
    return jax.shard_map(
        on_device,
        mesh=mesh,
        in_specs=(P("row", "col"), P()),
        out_specs=P("row", "col"),
        check_vma=False,
    )
```
